1024 devices in a mesh: gx: 16 (over x, y_hi), gy: 8 (over z), gz: 8 (over y_lo, core).
Axes of the slice: x: 8, y: 8 (y_hi: 2, y_lo: 4; y = y_hi * 4 + y_lo), z: 8, core: 2. Of those that a mesh axis runs over, the one named last changes fastest.
Arguments:
- density_scatter: float32 [64, 64, 1024], P('gx', 'gy', 'gz'), may hold values from 0.8 to 1.25
- initial_velocity: float32 [3, 64, 64, 1024], P(None, 'gx', 'gy', 'gz'), may hold values from -0.12 to 0.12
- bubble_mask: int32 [64, 64, 1024], P('gx', 'gy', 'gz'), may hold values from 0 to 1, as said below
- wall_flags: int32 [64, 64, 1024], P('gx', 'gy', 'gz'), may hold values 0 or 1
Outputs:
- density_field: float32 [64, 64, 1024], P('gx', 'gy', 'gz')
- velocity_field: float32 [3, 64, 64, 1024], P(None, 'gx', 'gy', 'gz')
The draws below stay inside these ranges and needn't reach their ends.
Inputs may be any that keep to these rules, and one draw needn't show every extreme that they name: `bubble_mask`: 1 at nodes inside a vapour bubble, 0 in the liquid. `wall_flags`: 1 at solid nodes, 0 at fluid nodes.
All inputs are finite; a program needn't handle non-finite values. No bound on the sum of `wall_flags` on one device may be relied on, other than what follows from the above.
Results may differ from the reference program's by a relative error of at most 0.0003.
Values sent between devices are 32-bit elements; how exact they have to be, the bound alone decides.
A program may use at most 32 MiB of HBM per device.

```python
import math
import jax
import jax.numpy as jnp
import numpy as np
from jax import lax

STEPS = 4
NX = 64
NY = 64
NZ = 1024


def spread_tiles(values):
    values = jnp.repeat(values, 8, axis=0)
    values = jnp.repeat(values, 8, axis=1)
    return jnp.repeat(values, 8, axis=2)


def draw_bubble_mask(key, part):
    key_centre, key_radius = jax.random.split(jax.random.fold_in(key, 17))
    tiles = (NX // 8, NY // 8, NZ // 8)
    centre = jax.random.randint(key_centre, tiles + (3,), 2, 6)
    radius = spread_tiles(jax.random.randint(key_radius, tiles, 1, 4))
    first = (jnp.arange(NX) % 8)[:, None, None] - spread_tiles(centre[..., 0])
    second = (jnp.arange(NY) % 8)[None, :, None] - spread_tiles(centre[..., 1])
    third = (jnp.arange(NZ) % 8)[None, None, :] - spread_tiles(centre[..., 2])
    distance = first * first + second * second + third * third
    return (distance <= radius * radius).astype(jnp.int32)


def touch_ends(drawn, stream_key, smallest, high):
    longest = drawn.shape.index(max(drawn.shape))
    spots = []
    for shift in (0, 1):
        where = [jax.random.randint(jax.random.fold_in(stream_key, axis), (), 0, length) for axis, length in enumerate(drawn.shape)]
        where[longest] = (where[longest] + shift) % drawn.shape[longest]
        spots.append(tuple(where))
    return drawn.at[spots[0]].set(smallest).at[spots[1]].set(high)


def steps_of(rng, extent, shards, least, top_value):
    level, own = 1.0, jax.random.fold_in(rng, 6)
    for position, blocks in shards:
        draws = jnp.exp(jax.random.uniform(jax.random.fold_in(own, position), (blocks,), jnp.float32, least / len(shards), top_value / len(shards)))
        level = level * jnp.repeat(draws, extent[position] // blocks).reshape([-1 if axis == position else 1 for axis in range(len(extent))])
    return level


def gaussian(own_key, dims, width, limit, pieces=(), kind=jnp.bfloat16):
    drawn = jax.random.normal(own_key, dims, jnp.float32) * width
    if len(pieces) > 0:
        drawn = steps_of(own_key, dims, pieces, -0.22, 0.18) * drawn
    return jnp.clip(drawn, min=-limit, max=limit).astype(kind)


def setup_inputs(seed: int = 0) -> dict:
    arg_keys = jax.random.split(jax.random.key(seed), 5)
    density_scatter = jnp.clip(jnp.exp(math.log(1.25) - 0.4462871 * jax.random.uniform(arg_keys[0], (NX, NY, NZ), jnp.float32) ** steps_of(arg_keys[0], (NX, NY, NZ), ((0, 16), (1, 8), (2, 8)), -0.2, 0.2)), 0.8, 1.25)
    initial_velocity = gaussian(arg_keys[1], (3, NX, NY, NZ), 0.04, 0.12, ((1, 16), (2, 8), (3, 8)), jnp.float32)
    bubble_mask = draw_bubble_mask(jax.random.fold_in(arg_keys[4], 71), 0)
    wall_flags = touch_ends((jax.random.randint(arg_keys[3], (NX, NY, NZ), 0, 16) < 1).astype(jnp.int32), jax.random.fold_in(arg_keys[3], 1), 0, 1)
    return dict(density_scatter=density_scatter, initial_velocity=initial_velocity, bubble_mask=bubble_mask, wall_flags=wall_flags)


lattice_velocities = np.array([[0, 0, 0], [1, 0, 0], [-1, 0, 0], [0, 1, 0], [0, -1, 0], [0, 0, 1], [0, 0, -1], [1, 1, 0], [-1, -1, 0], [1, -1, 0], [-1, 1, 0], [1, 0, 1], [-1, 0, -1], [1, 0, -1], [-1, 0, 1], [0, 1, 1], [0, -1, -1], [0, 1, -1], [0, -1, 1]])
weights = [1.0 / 3.0] + [1.0 / 18.0] * 6 + [1.0 / 36.0] * 12
opposite = [0, 2, 1, 4, 3, 6, 5, 8, 7, 10, 9, 12, 11, 14, 13, 16, 15, 18, 17]
liquid = 0.28
vapour = 0.06
wall_potential = 0.5
attractive_coupling = 1.0
critical_thermal_ratio = 0.06
viscous_rate = 1.25

def relaxation_matrix():
    table = lattice_velocities * 1.0
    first, second, third = (table[:, 0], table[:, 1], table[:, 2])
    squared_speed = first * first + second * second + third * third
    rows = [np.ones(19), 19.0 * squared_speed - 30.0, (21.0 * squared_speed * squared_speed - 53.0 * squared_speed + 24.0) / 2.0, first, (5.0 * squared_speed - 9.0) * first, second, (5.0 * squared_speed - 9.0) * second, third, (5.0 * squared_speed - 9.0) * third, 3.0 * first * first - squared_speed, (3.0 * squared_speed - 5.0) * (3.0 * first * first - squared_speed), second * second - third * third, (3.0 * squared_speed - 5.0) * (second * second - third * third), first * second, second * third, first * third, first * (second * second - third * third), second * (third * third - first * first), third * (first * first - second * second)]
    moment_space_vector = np.stack(rows)
    inverse_transform = moment_space_vector.T / np.sum(moment_space_vector * moment_space_vector, axis=1)
    rates = np.array([0.0, 1.19, 1.4, 0.0, 1.2, 0.0, 1.2, 0.0, 1.2, viscous_rate, 1.4, viscous_rate, 1.4, viscous_rate, viscous_rate, viscous_rate, 1.98, 1.98, 1.98])
    return inverse_transform * rates[None, :] @ moment_space_vector

def equilibrium(mass_per_volume, velocity):
    squared_speed = velocity[0] * velocity[0] + velocity[1] * velocity[1] + velocity[2] * velocity[2]
    rows = []
    for i in range(19):
        projection = float(lattice_velocities[i, 0]) * velocity[0] + float(lattice_velocities[i, 1]) * velocity[1] + float(lattice_velocities[i, 2]) * velocity[2]
        rows.append(weights[i] * mass_per_volume * (1.0 + 3.0 * projection + 4.5 * projection * projection - 1.5 * squared_speed))
    return jnp.stack(rows)

def moments(populations):
    return jnp.stack([sum((float(lattice_velocities[i, k]) * populations[i] for i in range(19) if lattice_velocities[i, k] != 0)) for k in range(3)])

def pseudo_potential(mass_per_volume):
    thermodynamic_stress = mass_per_volume * critical_thermal_ratio * (1.0 + mass_per_volume + mass_per_volume * mass_per_volume - mass_per_volume * mass_per_volume * mass_per_volume) / ((1.0 - mass_per_volume) * (1.0 - mass_per_volume) * (1.0 - mass_per_volume)) - attractive_coupling * mass_per_volume * mass_per_volume
    return jnp.sqrt(6.0 * (mass_per_volume / 3.0 - thermodynamic_stress))

def attraction(potential, nearby):
    parts = []
    for k in range(3):
        total = sum((weights[i] * float(lattice_velocities[i, k]) * nearby[i - 1] for i in range(1, 19) if lattice_velocities[i, k] != 0))
        parts.append(potential * total)
    return jnp.stack(parts)

def collide(populations, mass_per_volume, momentum, force, solid, kernel):
    velocity = momentum / mass_per_volume
    settled = equilibrium(mass_per_volume, velocity)
    pushed = equilibrium(mass_per_volume, velocity + force / mass_per_volume)
    relaxed = jnp.einsum('ij,jxyz->ixyz', kernel, populations - settled, precision=lax.Precision.HIGHEST)
    relaxed_distribution = populations - relaxed + pushed - settled
    bounced = populations[np.array(opposite)]
    return jnp.where(solid[None], bounced, relaxed_distribution)

def reference(density_scatter, initial_velocity, bubble_mask, wall_flags):
    kernel = jnp.asarray(relaxation_matrix(), jnp.float32)
    solid = wall_flags == 1
    mass_per_volume = jnp.where(bubble_mask == 1, vapour, liquid) * density_scatter
    populations = equilibrium(mass_per_volume, initial_velocity)
    for step in range(STEPS):
        mass_per_volume = lax.optimization_barrier(jnp.sum(populations, axis=0))
        momentum = moments(populations)
        potential = jnp.where(solid, wall_potential, pseudo_potential(mass_per_volume))
        nearby = [jnp.roll(potential, tuple((-int(v) for v in lattice_velocities[i])), axis=(0, 1, 2)) for i in range(1, 19)]
        force = attraction(potential, nearby)
        post = collide(populations, mass_per_volume, momentum, force, solid, kernel)
        populations = jnp.stack([jnp.roll(post[i], tuple((int(v) for v in lattice_velocities[i])), axis=(0, 1, 2)) for i in range(19)])
    mass_per_volume = lax.optimization_barrier(jnp.sum(populations, axis=0))
    momentum = moments(populations)
    density_field = jnp.where(solid, 0.0, mass_per_volume / liquid)
    velocity_field = jnp.where(solid[None], 0.0, math.sqrt(3.0) * momentum / mass_per_volume)
    return (density_field, velocity_field)
```

```python
import functools
import math

import jax
import jax.numpy as jnp
from jax import lax
from jax.experimental import pallas as pl
from jax.experimental.pallas import tpu as pltpu
from jax.sharding import PartitionSpec as P

STEPS = 4
MESH = pl.DeviceIdType.MESH
velocities = [
    (0, 0, 0),
    (1, 0, 0), (-1, 0, 0), (0, 1, 0), (0, -1, 0), (0, 0, 1), (0, 0, -1),
    (1, 1, 0), (-1, -1, 0), (1, -1, 0), (-1, 1, 0),
    (1, 0, 1), (-1, 0, -1), (1, 0, -1), (-1, 0, 1),
    (0, 1, 1), (0, -1, -1), (0, 1, -1), (0, -1, 1),
]
opposite = [0, 2, 1, 4, 3, 6, 5, 8, 7, 10, 9, 12, 11, 14, 13, 16, 15, 18, 17]
ROWS = 4
IN_ROWS = 24
OUT_ROWS = 16

offsets = [(1, 0), (-1, 0), (0, 1), (0, -1), (1, 1), (1, -1), (-1, 1), (-1, -1)]


def in_block(x, y, e):
    return x == e[0] and ROWS * e[1] <= y < ROWS * e[1] + ROWS


pops_of = {
    e: [
        (i, c)
        for c in range(ROWS)
        for i in range(19)
        if in_block(velocities[i][0], c + velocities[i][1], e)
    ]
    for e in offsets
}
start_of, total = {}, 0
for e in offsets:
    start_of[e] = total
    total += len(pops_of[e])
TOTAL = total


def pseudo_potential(rho):
    gap = 1.0 - rho
    square = rho * rho
    pressure = rho * 0.06 * (1.0 + rho + square - square * rho) / (gap * gap * gap) - square
    return jnp.sqrt(6.0 * (rho * (1.0 / 3.0) - pressure))


def equilibrium(rho, u):
    ux, uy, uz = u
    base = 1.0 - 1.5 * (ux * ux + uy * uy + uz * uz)
    third, axis, diagonal = rho * (1.0 / 3.0), rho * (1.0 / 18.0), rho * (1.0 / 36.0)
    out = [third * base]

    def pair(weight, projection):
        even = base + 4.5 * projection * projection
        odd = 3.0 * projection
        out.append(weight * (even + odd))
        out.append(weight * (even - odd))

    for value in (ux, uy, uz):
        pair(axis, value)
    for a, b in ((ux, uy), (ux, uz), (uy, uz)):
        pair(diagonal, a + b)
        pair(diagonal, a - b)
    return out


def density_and_momentum(f):
    s = {k: f[k] + f[k + 1] for k in range(1, 19, 2)}
    d = {k: f[k] - f[k + 1] for k in range(1, 19, 2)}
    rho = f[0] + (s[1] + s[3] + s[5]) + ((s[7] + s[9]) + (s[11] + s[13]) + (s[15] + s[17]))
    jx = d[1] + (d[7] + d[9]) + (d[11] + d[13])
    jy = d[3] + (d[7] - d[9]) + (d[15] + d[17])
    jz = d[5] + (d[11] - d[13]) + (d[15] - d[17])
    return rho, (jx, jy, jz)


def collide(f, force_over, solid):
    s = {k: f[k] + f[k + 1] for k in range(1, 19, 2)}
    d = {k: f[k] - f[k + 1] for k in range(1, 19, 2)}
    sx, sy, sz = s[1], s[3], s[5]
    sxy, sxz, syz = s[7] + s[9], s[11] + s[13], s[15] + s[17]
    pxy, pxz, pyz = s[7] - s[9], s[11] - s[13], s[15] - s[17]
    xy_x, xy_y = d[7] + d[9], d[7] - d[9]
    xz_x, xz_z = d[11] + d[13], d[11] - d[13]
    yz_y, yz_z = d[15] + d[17], d[15] - d[17]
    axes, diagonals = sx + sy + sz, sxy + sxz + syz
    rho = f[0] + axes + diagonals
    tx, ty, tz = xy_x + xz_x, xy_y + yz_y, xz_z + yz_z
    jx, jy, jz = d[1] + tx, d[3] + ty, d[5] + tz
    inverse = 1.0 / rho
    fx, fy, fz = force_over
    ux, uy, uz = jx * inverse, jy * inverse, jz * inverse
    vx, vy, vz = ux + fx * inverse, uy + fy * inverse, uz + fz * inverse
    exx, eyy, ezz = jx * ux, jy * uy, jz * uz
    exy, exz, eyz = jx * uy, jx * uz, jy * uz
    wx, wy, wz = rho * vx, rho * vy, rho * vz
    dxx, dyy, dzz = wx * vx - exx, wy * vy - eyy, wz * vz - ezz
    dxy, dxz, dyz = wx * vy - exy, wx * vz - exz, wy * vz - eyz
    e2, d2 = exx + eyy + ezz, dxx + dyy + dzz
    g_e = (1.19 * (-11.0 * rho + 19.0 * e2 - (-30.0 * f[0] - 11.0 * axes + 8.0 * diagonals)) + 19.0 * d2) * (1.0 / 2394.0)
    g_eps = (1.4 * (3.0 * rho - 5.5 * e2 - (12.0 * f[0] - 4.0 * axes + diagonals)) - 5.5 * d2) * (1.0 / 252.0)
    pxx_a, pxx_d = 3.0 * sx - axes, diagonals - 3.0 * syz
    pww_a, pww_d = sy - sz, sxy - sxz
    exx_e, dxx_e = 3.0 * exx - e2, 3.0 * dxx - d2
    eww_e, dww_e = eyy - ezz, dyy - dzz
    g_pxx = (1.25 * (exx_e - (pxx_a + pxx_d)) + dxx_e) * (1.0 / 36.0)
    g_pixx = (1.4 * (2.0 * pxx_a - pxx_d - 0.5 * exx_e) - 0.5 * dxx_e) * (1.0 / 72.0)
    g_pww = (1.25 * (eww_e - (pww_a + pww_d)) + dww_e) * (1.0 / 12.0)
    g_piww = (1.4 * (2.0 * pww_a - pww_d - 0.5 * eww_e) - 0.5 * dww_e) * (1.0 / 24.0)
    g_pxy = (1.25 * (exy - pxy) + dxy) * 0.25
    g_pxz = (1.25 * (exz - pxz) + dxz) * 0.25
    g_pyz = (1.25 * (eyz - pyz) + dyz) * 0.25

    def odd(j, axis, t, push):
        g_q = (1.2 * ((-2.0 / 3.0) * j + 4.0 * axis - t) - (2.0 / 3.0) * push) * (1.0 / 40.0)
        g_j = push * 0.1
        return g_j - 4.0 * g_q, g_j + g_q

    ax, bx = odd(jx, d[1], tx, fx)
    ay, by = odd(jy, d[3], ty, fy)
    az, bz = odd(jz, d[5], tz, fz)
    m = -1.98 / 8.0
    mx, my, mz = m * (xy_x - xz_x), m * (yz_y - xy_y), m * (xz_z - yz_z)
    axis_all = -11.0 * g_e - 4.0 * g_eps
    diagonal_all = 8.0 * g_e + g_eps
    part_x = g_pxx - 2.0 * g_pixx
    part_w = g_pww - 2.0 * g_piww
    even_x = axis_all + 2.0 * part_x
    even_y = axis_all - part_x + part_w
    even_z = axis_all - part_x - part_w
    both_x, both_w = g_pxx + g_pixx, g_pww + g_piww
    even_xy = diagonal_all + both_x + both_w
    even_xz = diagonal_all + both_x - both_w
    even_yz = diagonal_all - 2.0 * both_x
    cxy, cyx = bx + mx, by - my
    cxz, czx = bx - mx, bz + mz
    cyz, czy = by + my, bz - mz
    change = [12.0 * g_eps - 30.0 * g_e]

    def pair(even, odd_part):
        change.append(even + odd_part)
        change.append(even - odd_part)

    pair(even_x, ax)
    pair(even_y, ay)
    pair(even_z, az)
    pair(even_xy + g_pxy, cxy + cyx)
    pair(even_xy - g_pxy, cxy - cyx)
    pair(even_xz + g_pxz, cxz + czx)
    pair(even_xz - g_pxz, cxz - czx)
    pair(even_yz + g_pyz, cyz + czy)
    pair(even_yz - g_pyz, cyz - czy)
    return [jnp.where(solid, f[opposite[i]], f[i] + change[i]) for i in range(19)]


def kernel(
    sizes,
    scatter_hbm, speed_hbm, bubble_hbm, wall_hbm,
    density_out, velocity_out,
    scatter, speed, bubble, wall,
    in_send, in_recv, out_send, out_recv,
    psi, psi_x, psi_rest,
    pops, solids,
    send, recv,
    load_sem, in_sems, out_sems, psi_sems, round_sems,
):
    nx, ny, nz = sizes
    gx, gy, gz = lax.axis_index("gx"), lax.axis_index("gy"), lax.axis_index("gz")
    planes, groups = nx * 4, ny * 2
    X = gx * 4 + lax.div(gz, 2)
    Y = gy * 2 + lax.rem(gz, 2)

    def neighbour(e):
        x, y = lax.rem(X + (e[0] + planes), planes), lax.rem(Y + (e[1] + groups), groups)
        return {
            "gx": lax.div(x, 4),
            "gy": lax.div(y, 2),
            "gz": lax.rem(x, 4) * 2 + lax.rem(y, 2),
        }

    loads = [
        pltpu.make_async_copy(src, dst, load_sem.at[k])
        for k, (src, dst) in enumerate(
            ((scatter_hbm, scatter), (speed_hbm, speed), (bubble_hbm, bubble), (wall_hbm, wall))
        )
    ]
    for load in loads:
        load.start()
    barrier = pltpu.get_barrier_semaphore()
    where_to = [neighbour(e) for e in offsets]
    peers = [lax.rem(gz + k, nz) for k in range(1, nz)]
    for target in where_to + [{"gx": gx, "gy": gy, "gz": peer} for peer in peers]:
        pl.semaphore_signal(barrier, inc=1, device_id=target, device_id_type=MESH)
    for load in loads:
        load.wait()

    for p in range(4):
        rho0 = jnp.where(bubble[p] == 1, 0.06, 0.28) * scatter[p]
        solid = jnp.where(wall[p] == 1, 1.0, 0.0)
        fields = [rho0, speed[0, p], speed[1, p], speed[2, p], solid]
        for half in range(2):
            first = (p * 2 + half) * IN_ROWS
            for k, field in enumerate(fields):
                in_send[first + k * ROWS : first + (k + 1) * ROWS, :] = field[half * ROWS : (half + 1) * ROWS]
    pl.semaphore_wait(barrier, len(where_to) + len(peers))

    def exchange(source, target, rows, sems):
        mine = pl.ds(pl.multiple_of(gz * rows, 8), rows)
        copies = []
        for k, peer in enumerate(peers):
            copy = pltpu.make_async_remote_copy(
                src_ref=source.at[pl.ds(pl.multiple_of(peer * rows, 8), rows), :],
                dst_ref=target.at[mine, :],
                send_sem=sems.at[0, k],
                recv_sem=sems.at[1, k],
                device_id={"gx": gx, "gy": gy, "gz": peer},
                device_id_type=MESH,
            )
            copy.start()
            copies.append(copy)
        target[mine, :] = source[mine, :]
        for copy in copies:
            copy.wait()

    exchange(in_send, in_recv, IN_ROWS, in_sems)

    def line(field, c):
        return in_recv[pl.ds(field * ROWS + c, 8, stride=IN_ROWS), :]

    for c in range(ROWS):
        solids[c] = line(4, c)
        for i, value in enumerate(equilibrium(line(0, c), (line(1, c), line(2, c), line(3, c)))):
            pops[0, i, c] = value

    lane = lax.broadcasted_iota(jnp.int32, (8, 128), 1)
    is_first, is_last = lane == 0, lane == 127

    def shift(v, by):
        rolled = pltpu.roll(v, 1 if by > 0 else 127, 1)
        carried = pltpu.roll(rolled, 1 if by > 0 else 7, 0)
        return jnp.where(is_first if by > 0 else is_last, carried, rolled)

    def step(r, now, later):
        for c in range(ROWS):
            rho, _ = density_and_momentum([pops[now, i, c] for i in range(19)])
            psi[r, c] = jnp.where(solids[c] > 0.5, 0.5, pseudo_potential(rho))
        copies = []
        for k, e in enumerate(offsets):
            if e[1] == 0:
                source, target = psi.at[r], psi_x.at[r, k]
            else:
                source, target = psi.at[r, ROWS - 1 if e[1] > 0 else 0], psi_rest.at[r, k - 2]
            copies.append(
                pltpu.make_async_remote_copy(
                    src_ref=source,
                    dst_ref=target,
                    send_sem=psi_sems.at[0, r, k],
                    recv_sem=psi_sems.at[1, r, k],
                    device_id=where_to[k],
                    device_id_type=MESH,
                )
            )
            copies[-1].start()
        for copy in copies:
            copy.wait()

        def at(x, y):
            side = -1 if y < 0 else (1 if y >= ROWS else 0)
            if (x, side) == (0, 0):
                return psi[r, y]
            k = offsets.index((-x, -side))
            return psi_x[r, k, y] if side == 0 else psi_rest[r, k - 2]

        for c in range(ROWS):
            here = at(0, c)
            spread = [at(1, y) - at(-1, y) for y in (c - 1, c, c + 1)]
            left, middle, right = [at(x, c + 1) - at(x, c - 1) for x in (-1, 0, 1)]
            around = 2.0 * here + ((at(-1, c) + at(1, c)) + (at(0, c - 1) + at(0, c + 1)))
            scale = here * (1.0 / 36.0)
            force = (
                scale * ((2.0 * spread[1] + (spread[0] + spread[2])) + (shift(spread[1], 1) + shift(spread[1], -1))),
                scale * ((2.0 * middle + (left + right)) + (shift(middle, 1) + shift(middle, -1))),
                scale * (shift(around, -1) - shift(around, 1)),
            )
            post = collide([pops[now, i, c] for i in range(19)], force, solids[c] > 0.5)
            for i, (cx, cy, cz) in enumerate(velocities):
                value = shift(post[i], cz) if cz else post[i]
                if in_block(cx, c + cy, (0, 0)):
                    pops[later, i, c + cy] = value
                else:
                    for e in offsets:
                        if in_block(cx, c + cy, e):
                            send[r, start_of[e] + pops_of[e].index((i, c))] = value
        copies = []
        for k, e in enumerate(offsets):
            part = pl.ds(start_of[e], len(pops_of[e]))
            copies.append(
                pltpu.make_async_remote_copy(
                    src_ref=send.at[r, part],
                    dst_ref=recv.at[r, part],
                    send_sem=round_sems.at[0, r, k],
                    recv_sem=round_sems.at[1, r, k],
                    device_id=where_to[k],
                    device_id_type=MESH,
                )
            )
            copies[-1].start()
        for copy in copies:
            copy.wait()
        for e in offsets:
            for k, (i, c) in enumerate(pops_of[e]):
                pops[later, i, c + velocities[i][1] - ROWS * e[1]] = recv[r, start_of[e] + k]

    def body(r, carry):
        now = lax.rem(r, 2)
        step(r, now, 1 - now)
        return carry

    lax.fori_loop(0, STEPS, body, 0)

    for c in range(ROWS):
        rho, momentum = density_and_momentum([pops[STEPS % 2, i, c] for i in range(19)])
        fluid = solids[c] < 0.5
        scale = math.sqrt(3.0) / rho
        fields = [rho * (1.0 / 0.28)] + [j * scale for j in momentum]
        for k, field in enumerate(fields):
            out_send[pl.ds(k * ROWS + c, 8, stride=OUT_ROWS), :] = jnp.where(fluid, field, 0.0)
    exchange(out_send, out_recv, OUT_ROWS, out_sems)
    for p in range(4):
        for half in range(2):
            first = (p * 2 + half) * OUT_ROWS
            rows = slice(half * ROWS, (half + 1) * ROWS)
            density_out[p, rows, :] = out_recv[first : first + ROWS, :]
            for k in range(3):
                velocity_out[k, p, rows, :] = out_recv[first + (k + 1) * ROWS : first + (k + 2) * ROWS, :]


def solution(mesh):
    sizes = (mesh.shape["gx"], mesh.shape["gy"], mesh.shape["gz"])
    block = (4, 8, 128)
    tile = (8, 128)

    def on_device(density_scatter, initial_velocity, bubble_mask, wall_flags):
        return tuple(
            pl.pallas_call(
                functools.partial(kernel, sizes),
                out_shape=[
                    jax.ShapeDtypeStruct(block, jnp.float32),
                    jax.ShapeDtypeStruct((3,) + block, jnp.float32),
                ],
                in_specs=[pl.BlockSpec(memory_space=pl.ANY)] * 4,
                out_specs=[pl.BlockSpec(memory_space=pltpu.VMEM)] * 2,
                scratch_shapes=[
                    pltpu.VMEM(block, jnp.float32),
                    pltpu.VMEM((3,) + block, jnp.float32),
                    pltpu.VMEM(block, jnp.int32),
                    pltpu.VMEM(block, jnp.int32),
                    pltpu.VMEM((8 * IN_ROWS, 128), jnp.float32),
                    pltpu.VMEM((8 * IN_ROWS, 128), jnp.float32),
                    pltpu.VMEM((8 * OUT_ROWS, 128), jnp.float32),
                    pltpu.VMEM((8 * OUT_ROWS, 128), jnp.float32),
                    pltpu.VMEM((STEPS, ROWS) + tile, jnp.float32),
                    pltpu.VMEM((STEPS, 2, ROWS) + tile, jnp.float32),
                    pltpu.VMEM((STEPS, 6) + tile, jnp.float32),
                    pltpu.VMEM((2, 19, ROWS) + tile, jnp.float32),
                    pltpu.VMEM((ROWS,) + tile, jnp.float32),
                    pltpu.VMEM((STEPS, TOTAL) + tile, jnp.float32),
                    pltpu.VMEM((STEPS, TOTAL) + tile, jnp.float32),
                    pltpu.SemaphoreType.DMA((4,)),
                    pltpu.SemaphoreType.DMA((2, 7)),
                    pltpu.SemaphoreType.DMA((2, 7)),
                    pltpu.SemaphoreType.DMA((2, STEPS, 8)),
                    pltpu.SemaphoreType.DMA((2, STEPS, 8)),
                ],
                compiler_params=pltpu.CompilerParams(collective_id=0, has_side_effects=True),
            )(density_scatter, initial_velocity, bubble_mask, wall_flags)
        )

    return jax.shard_map(
        on_device,
        mesh=mesh,
        in_specs=(
            P("gx", "gy", "gz"),
            P(None, "gx", "gy", "gz"),
            P("gx", "gy", "gz"),
            P("gx", "gy", "gz"),
        ),
        out_specs=(P("gx", "gy", "gz"), P(None, "gx", "gy", "gz")),
        check_vma=False,
    )
```

```python
import functools
import math

import jax
import jax.numpy as jnp
from jax import lax
from jax.experimental import pallas as pl
from jax.experimental.pallas import tpu as pltpu
from jax.sharding import PartitionSpec as P

STEPS = 4
MESH = pl.DeviceIdType.MESH
velocities = [
    (0, 0, 0),
    (1, 0, 0), (-1, 0, 0), (0, 1, 0), (0, -1, 0), (0, 0, 1), (0, 0, -1),
    (1, 1, 0), (-1, -1, 0), (1, -1, 0), (-1, 1, 0),
    (1, 0, 1), (-1, 0, -1), (1, 0, -1), (-1, 0, 1),
    (0, 1, 1), (0, -1, -1), (0, 1, -1), (0, -1, 1),
]
opposite = [0, 2, 1, 4, 3, 6, 5, 8, 7, 10, 9, 12, 11, 14, 13, 16, 15, 18, 17]
ROWS = 4
IN_ROWS = 24
OUT_ROWS = 16

offsets = [(1, 0), (-1, 0), (0, 1), (0, -1), (1, 1), (1, -1), (-1, 1), (-1, -1)]
far = [(2, 1), (2, -1), (-2, 1), (-2, -1), (2, 0), (-2, 0)]


def in_block(x, y, e):
    return x == e[0] and ROWS * e[1] <= y < ROWS * e[1] + ROWS


def in_halo(x, y, e):
    near = abs(x - e[0]) <= 1 and ROWS * e[1] - 1 <= y <= ROWS * e[1] + ROWS
    return near and not in_block(x, y, e)


pops_of = {
    e: [
        (i, c)
        for c in range(ROWS)
        for i in range(19)
        if in_block(velocities[i][0], c + velocities[i][1], e)
    ]
    for e in offsets + far
}
shares_of = {
    e: [(x, y) for x in (-1, 0, 1) for y in range(-1, ROWS + 1) if in_halo(x, y, e)]
    for e in offsets + far
}
start_of, total = {}, 0
for e in offsets + far:
    start_of[e] = total
    total += len(pops_of[e]) + len(shares_of[e])
TOTAL = total


def pseudo_potential(rho):
    gap = 1.0 - rho
    square = rho * rho
    pressure = rho * 0.06 * (1.0 + rho + square - square * rho) / (gap * gap * gap) - square
    return jnp.sqrt(6.0 * (rho * (1.0 / 3.0) - pressure))


def equilibrium(rho, u):
    ux, uy, uz = u
    base = 1.0 - 1.5 * (ux * ux + uy * uy + uz * uz)
    third, axis, diagonal = rho * (1.0 / 3.0), rho * (1.0 / 18.0), rho * (1.0 / 36.0)
    out = [third * base]

    def pair(weight, projection):
        even = base + 4.5 * projection * projection
        odd = 3.0 * projection
        out.append(weight * (even + odd))
        out.append(weight * (even - odd))

    for value in (ux, uy, uz):
        pair(axis, value)
    for a, b in ((ux, uy), (ux, uz), (uy, uz)):
        pair(diagonal, a + b)
        pair(diagonal, a - b)
    return out


def density_and_momentum(f):
    s = {k: f[k] + f[k + 1] for k in range(1, 19, 2)}
    d = {k: f[k] - f[k + 1] for k in range(1, 19, 2)}
    rho = f[0] + (s[1] + s[3] + s[5]) + ((s[7] + s[9]) + (s[11] + s[13]) + (s[15] + s[17]))
    jx = d[1] + (d[7] + d[9]) + (d[11] + d[13])
    jy = d[3] + (d[7] - d[9]) + (d[15] + d[17])
    jz = d[5] + (d[11] - d[13]) + (d[15] - d[17])
    return rho, (jx, jy, jz)


def collide(f, force_over, solid):
    s = {k: f[k] + f[k + 1] for k in range(1, 19, 2)}
    d = {k: f[k] - f[k + 1] for k in range(1, 19, 2)}
    sx, sy, sz = s[1], s[3], s[5]
    sxy, sxz, syz = s[7] + s[9], s[11] + s[13], s[15] + s[17]
    pxy, pxz, pyz = s[7] - s[9], s[11] - s[13], s[15] - s[17]
    xy_x, xy_y = d[7] + d[9], d[7] - d[9]
    xz_x, xz_z = d[11] + d[13], d[11] - d[13]
    yz_y, yz_z = d[15] + d[17], d[15] - d[17]
    axes, diagonals = sx + sy + sz, sxy + sxz + syz
    rho = f[0] + axes + diagonals
    tx, ty, tz = xy_x + xz_x, xy_y + yz_y, xz_z + yz_z
    jx, jy, jz = d[1] + tx, d[3] + ty, d[5] + tz
    inverse = 1.0 / rho
    fx, fy, fz = force_over
    ux, uy, uz = jx * inverse, jy * inverse, jz * inverse
    vx, vy, vz = ux + fx * inverse, uy + fy * inverse, uz + fz * inverse
    exx, eyy, ezz = jx * ux, jy * uy, jz * uz
    exy, exz, eyz = jx * uy, jx * uz, jy * uz
    wx, wy, wz = rho * vx, rho * vy, rho * vz
    dxx, dyy, dzz = wx * vx - exx, wy * vy - eyy, wz * vz - ezz
    dxy, dxz, dyz = wx * vy - exy, wx * vz - exz, wy * vz - eyz
    e2, d2 = exx + eyy + ezz, dxx + dyy + dzz
    g_e = (1.19 * (-11.0 * rho + 19.0 * e2 - (-30.0 * f[0] - 11.0 * axes + 8.0 * diagonals)) + 19.0 * d2) * (1.0 / 2394.0)
    g_eps = (1.4 * (3.0 * rho - 5.5 * e2 - (12.0 * f[0] - 4.0 * axes + diagonals)) - 5.5 * d2) * (1.0 / 252.0)
    pxx_a, pxx_d = 3.0 * sx - axes, diagonals - 3.0 * syz
    pww_a, pww_d = sy - sz, sxy - sxz
    exx_e, dxx_e = 3.0 * exx - e2, 3.0 * dxx - d2
    eww_e, dww_e = eyy - ezz, dyy - dzz
    g_pxx = (1.25 * (exx_e - (pxx_a + pxx_d)) + dxx_e) * (1.0 / 36.0)
    g_pixx = (1.4 * (2.0 * pxx_a - pxx_d - 0.5 * exx_e) - 0.5 * dxx_e) * (1.0 / 72.0)
    g_pww = (1.25 * (eww_e - (pww_a + pww_d)) + dww_e) * (1.0 / 12.0)
    g_piww = (1.4 * (2.0 * pww_a - pww_d - 0.5 * eww_e) - 0.5 * dww_e) * (1.0 / 24.0)
    g_pxy = (1.25 * (exy - pxy) + dxy) * 0.25
    g_pxz = (1.25 * (exz - pxz) + dxz) * 0.25
    g_pyz = (1.25 * (eyz - pyz) + dyz) * 0.25

    def odd(j, axis, t, push):
        g_q = (1.2 * ((-2.0 / 3.0) * j + 4.0 * axis - t) - (2.0 / 3.0) * push) * (1.0 / 40.0)
        g_j = push * 0.1
        return g_j - 4.0 * g_q, g_j + g_q

    ax, bx = odd(jx, d[1], tx, fx)
    ay, by = odd(jy, d[3], ty, fy)
    az, bz = odd(jz, d[5], tz, fz)
    m = -1.98 / 8.0
    mx, my, mz = m * (xy_x - xz_x), m * (yz_y - xy_y), m * (xz_z - yz_z)
    axis_all = -11.0 * g_e - 4.0 * g_eps
    diagonal_all = 8.0 * g_e + g_eps
    part_x = g_pxx - 2.0 * g_pixx
    part_w = g_pww - 2.0 * g_piww
    even_x = axis_all + 2.0 * part_x
    even_y = axis_all - part_x + part_w
    even_z = axis_all - part_x - part_w
    both_x, both_w = g_pxx + g_pixx, g_pww + g_piww
    even_xy = diagonal_all + both_x + both_w
    even_xz = diagonal_all + both_x - both_w
    even_yz = diagonal_all - 2.0 * both_x
    cxy, cyx = bx + mx, by - my
    cxz, czx = bx - mx, bz + mz
    cyz, czy = by + my, bz - mz
    change = [12.0 * g_eps - 30.0 * g_e]

    def pair(even, odd_part):
        change.append(even + odd_part)
        change.append(even - odd_part)

    pair(even_x, ax)
    pair(even_y, ay)
    pair(even_z, az)
    pair(even_xy + g_pxy, cxy + cyx)
    pair(even_xy - g_pxy, cxy - cyx)
    pair(even_xz + g_pxz, cxz + czx)
    pair(even_xz - g_pxz, cxz - czx)
    pair(even_yz + g_pyz, cyz + czy)
    pair(even_yz - g_pyz, cyz - czy)
    return [jnp.where(solid, f[opposite[i]], f[i] + change[i]) for i in range(19)]


def kernel(
    sizes,
    scatter_hbm, speed_hbm, bubble_hbm, wall_hbm,
    fields_out,
    scatter, speed, bubble, wall,
    in_send, in_recv, out_send, out_recv,
    edge_send, edge_x, edge_rest,
    pops, psi, solids,
    send, recv,
    load_sem, in_sems, out_sems, edge_sems, round_sems,
):
    nx, ny, nz = sizes
    gx, gy, gz = lax.axis_index("gx"), lax.axis_index("gy"), lax.axis_index("gz")
    planes, groups = nx * 4, ny * 2
    X = gx * 4 + lax.div(gz, 2)
    Y = gy * 2 + lax.rem(gz, 2)

    def neighbour(e):
        x, y = lax.rem(X + (e[0] + planes), planes), lax.rem(Y + (e[1] + groups), groups)
        return {
            "gx": lax.div(x, 4),
            "gy": lax.div(y, 2),
            "gz": lax.rem(x, 4) * 2 + lax.rem(y, 2),
        }

    loads = [
        pltpu.make_async_copy(src, dst, load_sem.at[k])
        for k, (src, dst) in enumerate(
            ((scatter_hbm, scatter), (speed_hbm, speed), (bubble_hbm, bubble), (wall_hbm, wall))
        )
    ]
    for load in loads:
        load.start()
    barrier = pltpu.get_barrier_semaphore()
    where_to = [neighbour(e) for e in offsets + far]
    peers = [lax.rem(gz + k, nz) for k in range(1, nz)]
    for target in where_to + [{"gx": gx, "gy": gy, "gz": peer} for peer in peers]:
        pl.semaphore_signal(barrier, inc=1, device_id=target, device_id_type=MESH)
    for load in loads:
        load.wait()

    for p in range(4):
        rho0 = jnp.where(bubble[p] == 1, 0.06, 0.28) * scatter[p]
        solid = jnp.where(wall[p] == 1, 1.0, 0.0)
        fields = [rho0, speed[0, p], speed[1, p], speed[2, p], solid]
        for half in range(2):
            first = (p * 2 + half) * IN_ROWS
            for k, field in enumerate(fields):
                in_send[first + k * ROWS : first + (k + 1) * ROWS, :] = field[half * ROWS : (half + 1) * ROWS]
    pl.semaphore_wait(barrier, len(where_to) + len(peers))

    def exchange(source, target, rows, sems):
        mine = pl.ds(pl.multiple_of(gz * rows, 8), rows)
        copies = []
        for k, peer in enumerate(peers):
            copy = pltpu.make_async_remote_copy(
                src_ref=source.at[pl.ds(pl.multiple_of(peer * rows, 8), rows), :],
                dst_ref=target.at[mine, :],
                send_sem=sems.at[0, k],
                recv_sem=sems.at[1, k],
                device_id={"gx": gx, "gy": gy, "gz": peer},
                device_id_type=MESH,
            )
            copy.start()
            copies.append(copy)
        target[mine, :] = source[mine, :]
        for copy in copies:
            copy.wait()

    exchange(in_send, in_recv, IN_ROWS, in_sems)

    def line(field, c):
        return in_recv[pl.ds(field * ROWS + c, 8, stride=IN_ROWS), :]

    for c in range(ROWS):
        solid = line(4, c)
        solids[1, c + 1] = solid
        edge_send[c, 0] = jnp.where(solid > 0.5, 0.5, pseudo_potential(line(0, c)))
        edge_send[c, 1] = solid
    copies = []
    for k, e in enumerate(offsets):
        if e[1] == 0:
            source, target = edge_send, edge_x.at[k]
        else:
            source, target = edge_send.at[ROWS - 1 if e[1] > 0 else 0], edge_rest.at[k - 2]
        copies.append(
            pltpu.make_async_remote_copy(
                src_ref=source,
                dst_ref=target,
                send_sem=edge_sems.at[0, k],
                recv_sem=edge_sems.at[1, k],
                device_id=where_to[k],
                device_id_type=MESH,
            )
        )
        copies[-1].start()
    for c in range(ROWS):
        for i, value in enumerate(equilibrium(line(0, c), (line(1, c), line(2, c), line(3, c)))):
            pops[0, i, c] = value
    for copy in copies:
        copy.wait()
    for k, e in enumerate(offsets):
        if e[1] == 0:
            for c in range(ROWS):
                psi[1 - e[0], c + 1] = edge_x[k, c, 0]
                solids[1 - e[0], c + 1] = edge_x[k, c, 1]
        else:
            y = 0 if e[1] > 0 else ROWS + 1
            psi[1 - e[0], y] = edge_rest[k - 2, 0]
            solids[1 - e[0], y] = edge_rest[k - 2, 1]

    lane = lax.broadcasted_iota(jnp.int32, (8, 128), 1)
    is_first, is_last = lane == 0, lane == 127

    def shift(v, by):
        rolled = pltpu.roll(v, 1 if by > 0 else 127, 1)
        carried = pltpu.roll(rolled, 1 if by > 0 else 7, 0)
        return jnp.where(is_first if by > 0 else is_last, carried, rolled)

    halo = [(x, y) for x in (-1, 0, 1) for y in range(-1, ROWS + 1) if in_halo(x, y, (0, 0))]

    def at(x, y):
        return psi[x + 1, y + 1]

    def potential_of(x, y, rho):
        psi[x + 1, y + 1] = jnp.where(solids[x + 1, y + 1] > 0.5, 0.5, pseudo_potential(rho))

    def step(r, now, later, last):
        for c in range(ROWS):
            potential_of(0, c, density_and_momentum([pops[now, i, c] for i in range(19)])[0])
        share = {}
        for c in range(ROWS):
            here = at(0, c)
            spread = [at(1, y) - at(-1, y) for y in (c - 1, c, c + 1)]
            left, middle, right = [at(x, c + 1) - at(x, c - 1) for x in (-1, 0, 1)]
            around = 2.0 * here + ((at(-1, c) + at(1, c)) + (at(0, c - 1) + at(0, c + 1)))
            scale = here * (1.0 / 36.0)
            force = (
                scale * ((2.0 * spread[1] + (spread[0] + spread[2])) + (shift(spread[1], 1) + shift(spread[1], -1))),
                scale * ((2.0 * middle + (left + right)) + (shift(middle, 1) + shift(middle, -1))),
                scale * (shift(around, -1) - shift(around, 1)),
            )
            post = collide([pops[now, i, c] for i in range(19)], force, solids[1, c + 1] > 0.5)
            for i, (cx, cy, cz) in enumerate(velocities):
                value = shift(post[i], cz) if cz else post[i]
                node = cx, c + cy
                if not last:
                    share[node] = share[node] + value if node in share else value
                if in_block(*node, (0, 0)):
                    pops[later, i, c + cy] = value
                else:
                    for e in offsets:
                        if in_block(*node, e):
                            send[r, start_of[e] + pops_of[e].index((i, c))] = value
        copies = []
        for k, e in enumerate(offsets if last else offsets + far):
            part = pl.ds(start_of[e], len(pops_of[e]))
            if not last:
                first = start_of[e] + len(pops_of[e])
                for n, node in enumerate(shares_of[e]):
                    send[r, first + n] = share[node]
                part = pl.ds(start_of[e], len(pops_of[e]) + len(shares_of[e]))
            copies.append(
                pltpu.make_async_remote_copy(
                    src_ref=send.at[r, part],
                    dst_ref=recv.at[r, part],
                    send_sem=round_sems.at[0, r, k],
                    recv_sem=round_sems.at[1, r, k],
                    device_id=where_to[k],
                    device_id_type=MESH,
                )
            )
            copies[-1].start()
        for copy in copies:
            copy.wait()
        for e in offsets:
            for k, (i, c) in enumerate(pops_of[e]):
                pops[later, i, c + velocities[i][1] - ROWS * e[1]] = recv[r, start_of[e] + k]
        if not last:
            for x, y in halo:
                rho = share[x, y]
                for e in offsets + far:
                    there = (x + e[0], y + ROWS * e[1])
                    if there in shares_of[e]:
                        rho = rho + recv[r, start_of[e] + len(pops_of[e]) + shares_of[e].index(there)]
                potential_of(x, y, rho)

    def body(r, carry):
        now = lax.rem(r, 2)
        step(r, now, 1 - now, False)
        return carry

    lax.fori_loop(0, STEPS - 1, body, 0)
    step(STEPS - 1, (STEPS - 1) % 2, STEPS % 2, True)

    for c in range(ROWS):
        rho, momentum = density_and_momentum([pops[STEPS % 2, i, c] for i in range(19)])
        fluid = solids[1, c + 1] < 0.5
        scale = math.sqrt(3.0) / rho
        fields = [rho * (1.0 / 0.28)] + [j * scale for j in momentum]
        for k, field in enumerate(fields):
            out_send[pl.ds(k * ROWS + c, 8, stride=OUT_ROWS), :] = jnp.where(fluid, field, 0.0)
    exchange(out_send, out_recv, OUT_ROWS, out_sems)
    for p in range(4):
        for half in range(2):
            first = (p * 2 + half) * OUT_ROWS
            rows = slice(half * ROWS, (half + 1) * ROWS)
            for k in range(4):
                fields_out[k, p, rows, :] = out_recv[first + k * ROWS : first + (k + 1) * ROWS, :]


def solution(mesh):
    sizes = (mesh.shape["gx"], mesh.shape["gy"], mesh.shape["gz"])
    block = (4, 8, 128)
    tile = (8, 128)

    def on_device(density_scatter, initial_velocity, bubble_mask, wall_flags):
        fields = pl.pallas_call(
                functools.partial(kernel, sizes),
                out_shape=jax.ShapeDtypeStruct((4,) + block, jnp.float32),
                in_specs=[pl.BlockSpec(memory_space=pl.ANY)] * 4,
                out_specs=pl.BlockSpec(memory_space=pltpu.VMEM),
                scratch_shapes=[
                    pltpu.VMEM(block, jnp.float32),
                    pltpu.VMEM((3,) + block, jnp.float32),
                    pltpu.VMEM(block, jnp.int32),
                    pltpu.VMEM(block, jnp.int32),
                    pltpu.VMEM((8 * IN_ROWS, 128), jnp.float32),
                    pltpu.VMEM((8 * IN_ROWS, 128), jnp.float32),
                    pltpu.VMEM((8 * OUT_ROWS, 128), jnp.float32),
                    pltpu.VMEM((8 * OUT_ROWS, 128), jnp.float32),
                    pltpu.VMEM((ROWS, 2) + tile, jnp.float32),
                    pltpu.VMEM((2, ROWS, 2) + tile, jnp.float32),
                    pltpu.VMEM((6, 2) + tile, jnp.float32),
                    pltpu.VMEM((2, 19, ROWS) + tile, jnp.float32),
                    pltpu.VMEM((3, ROWS + 2) + tile, jnp.float32),
                    pltpu.VMEM((3, ROWS + 2) + tile, jnp.float32),
                    pltpu.VMEM((STEPS, TOTAL) + tile, jnp.float32),
                    pltpu.VMEM((STEPS, TOTAL) + tile, jnp.float32),
                    pltpu.SemaphoreType.DMA((4,)),
                    pltpu.SemaphoreType.DMA((2, 7)),
                    pltpu.SemaphoreType.DMA((2, 7)),
                    pltpu.SemaphoreType.DMA((2, 8)),
                    pltpu.SemaphoreType.DMA((2, STEPS, 14)),
                ],
                compiler_params=pltpu.CompilerParams(collective_id=0, has_side_effects=True),
            )(density_scatter, initial_velocity, bubble_mask, wall_flags)
        return fields[0], fields[1:]

    return jax.shard_map(
        on_device,
        mesh=mesh,
        in_specs=(
            P("gx", "gy", "gz"),
            P(None, "gx", "gy", "gz"),
            P("gx", "gy", "gz"),
            P("gx", "gy", "gz"),
        ),
        out_specs=(P("gx", "gy", "gz"), P(None, "gx", "gy", "gz")),
        check_vma=False,
    )
```

```python
import functools
import math

import jax
import jax.numpy as jnp
from jax import lax
from jax.experimental import pallas as pl
from jax.experimental.pallas import tpu as pltpu
from jax.sharding import PartitionSpec as P

STEPS = 4
MESH = pl.DeviceIdType.MESH
velocities = [
    (0, 0, 0),
    (1, 0, 0), (-1, 0, 0), (0, 1, 0), (0, -1, 0), (0, 0, 1), (0, 0, -1),
    (1, 1, 0), (-1, -1, 0), (1, -1, 0), (-1, 1, 0),
    (1, 0, 1), (-1, 0, -1), (1, 0, -1), (-1, 0, 1),
    (0, 1, 1), (0, -1, -1), (0, 1, -1), (0, -1, 1),
]
opposite = [0, 2, 1, 4, 3, 6, 5, 8, 7, 10, 9, 12, 11, 14, 13, 16, 15, 18, 17]
ROWS = 4
IN_ROWS = 24
OUT_ROWS = 16

offsets = [(1, 0), (-1, 0), (0, 1), (0, -1), (1, 1), (1, -1), (-1, 1), (-1, -1)]
far = [(2, 1), (2, -1), (-2, 1), (-2, -1), (2, 0), (-2, 0)]


def in_block(x, y, e):
    return x == e[0] and ROWS * e[1] <= y < ROWS * e[1] + ROWS


def in_halo(x, y, e):
    near = abs(x - e[0]) <= 1 and ROWS * e[1] - 1 <= y <= ROWS * e[1] + ROWS
    return near and not in_block(x, y, e)


pops_of = {
    e: [
        (i, c)
        for c in range(ROWS)
        for i in range(19)
        if in_block(velocities[i][0], c + velocities[i][1], e)
    ]
    for e in offsets + far
}
shares_of = {
    e: [(x, y) for x in (-1, 0, 1) for y in range(-1, ROWS + 1) if in_halo(x, y, e)]
    for e in offsets + far
}
start_of, total = {}, 0
for e in offsets + far:
    start_of[e] = total
    total += len(pops_of[e]) + len(shares_of[e])
TOTAL = total


def pseudo_potential(rho):
    gap = 1.0 - rho
    square = rho * rho
    pressure = rho * 0.06 * (1.0 + rho + square - square * rho) / (gap * gap * gap) - square
    return jnp.sqrt(6.0 * (rho * (1.0 / 3.0) - pressure))


def equilibrium(rho, u):
    ux, uy, uz = u
    base = 1.0 - 1.5 * (ux * ux + uy * uy + uz * uz)
    third, axis, diagonal = rho * (1.0 / 3.0), rho * (1.0 / 18.0), rho * (1.0 / 36.0)
    out = [third * base]

    def pair(weight, projection):
        even = base + 4.5 * projection * projection
        odd = 3.0 * projection
        out.append(weight * (even + odd))
        out.append(weight * (even - odd))

    for value in (ux, uy, uz):
        pair(axis, value)
    for a, b in ((ux, uy), (ux, uz), (uy, uz)):
        pair(diagonal, a + b)
        pair(diagonal, a - b)
    return out


def density_and_momentum(f):
    s = {k: f[k] + f[k + 1] for k in range(1, 19, 2)}
    d = {k: f[k] - f[k + 1] for k in range(1, 19, 2)}
    rho = f[0] + (s[1] + s[3] + s[5]) + ((s[7] + s[9]) + (s[11] + s[13]) + (s[15] + s[17]))
    jx = d[1] + (d[7] + d[9]) + (d[11] + d[13])
    jy = d[3] + (d[7] - d[9]) + (d[15] + d[17])
    jz = d[5] + (d[11] - d[13]) + (d[15] - d[17])
    return rho, (jx, jy, jz)


def collide(f, force_over, solid):
    s = {k: f[k] + f[k + 1] for k in range(1, 19, 2)}
    d = {k: f[k] - f[k + 1] for k in range(1, 19, 2)}
    sx, sy, sz = s[1], s[3], s[5]
    sxy, sxz, syz = s[7] + s[9], s[11] + s[13], s[15] + s[17]
    pxy, pxz, pyz = s[7] - s[9], s[11] - s[13], s[15] - s[17]
    xy_x, xy_y = d[7] + d[9], d[7] - d[9]
    xz_x, xz_z = d[11] + d[13], d[11] - d[13]
    yz_y, yz_z = d[15] + d[17], d[15] - d[17]
    axes, diagonals = sx + sy + sz, sxy + sxz + syz
    rho = f[0] + axes + diagonals
    tx, ty, tz = xy_x + xz_x, xy_y + yz_y, xz_z + yz_z
    jx, jy, jz = d[1] + tx, d[3] + ty, d[5] + tz
    inverse = 1.0 / rho
    fx, fy, fz = force_over
    ux, uy, uz = jx * inverse, jy * inverse, jz * inverse
    vx, vy, vz = ux + fx * inverse, uy + fy * inverse, uz + fz * inverse
    exx, eyy, ezz = jx * ux, jy * uy, jz * uz
    exy, exz, eyz = jx * uy, jx * uz, jy * uz
    wx, wy, wz = rho * vx, rho * vy, rho * vz
    dxx, dyy, dzz = wx * vx - exx, wy * vy - eyy, wz * vz - ezz
    dxy, dxz, dyz = wx * vy - exy, wx * vz - exz, wy * vz - eyz
    e2, d2 = exx + eyy + ezz, dxx + dyy + dzz
    g_e = (1.19 * (-11.0 * rho + 19.0 * e2 - (-30.0 * f[0] - 11.0 * axes + 8.0 * diagonals)) + 19.0 * d2) * (1.0 / 2394.0)
    g_eps = (1.4 * (3.0 * rho - 5.5 * e2 - (12.0 * f[0] - 4.0 * axes + diagonals)) - 5.5 * d2) * (1.0 / 252.0)
    pxx_a, pxx_d = 3.0 * sx - axes, diagonals - 3.0 * syz
    pww_a, pww_d = sy - sz, sxy - sxz
    exx_e, dxx_e = 3.0 * exx - e2, 3.0 * dxx - d2
    eww_e, dww_e = eyy - ezz, dyy - dzz
    g_pxx = (1.25 * (exx_e - (pxx_a + pxx_d)) + dxx_e) * (1.0 / 36.0)
    g_pixx = (1.4 * (2.0 * pxx_a - pxx_d - 0.5 * exx_e) - 0.5 * dxx_e) * (1.0 / 72.0)
    g_pww = (1.25 * (eww_e - (pww_a + pww_d)) + dww_e) * (1.0 / 12.0)
    g_piww = (1.4 * (2.0 * pww_a - pww_d - 0.5 * eww_e) - 0.5 * dww_e) * (1.0 / 24.0)
    g_pxy = (1.25 * (exy - pxy) + dxy) * 0.25
    g_pxz = (1.25 * (exz - pxz) + dxz) * 0.25
    g_pyz = (1.25 * (eyz - pyz) + dyz) * 0.25

    def odd(j, axis, t, push):
        g_q = (1.2 * ((-2.0 / 3.0) * j + 4.0 * axis - t) - (2.0 / 3.0) * push) * (1.0 / 40.0)
        g_j = push * 0.1
        return g_j - 4.0 * g_q, g_j + g_q

    ax, bx = odd(jx, d[1], tx, fx)
    ay, by = odd(jy, d[3], ty, fy)
    az, bz = odd(jz, d[5], tz, fz)
    m = -1.98 / 8.0
    mx, my, mz = m * (xy_x - xz_x), m * (yz_y - xy_y), m * (xz_z - yz_z)
    axis_all = -11.0 * g_e - 4.0 * g_eps
    diagonal_all = 8.0 * g_e + g_eps
    part_x = g_pxx - 2.0 * g_pixx
    part_w = g_pww - 2.0 * g_piww
    even_x = axis_all + 2.0 * part_x
    even_y = axis_all - part_x + part_w
    even_z = axis_all - part_x - part_w
    both_x, both_w = g_pxx + g_pixx, g_pww + g_piww
    even_xy = diagonal_all + both_x + both_w
    even_xz = diagonal_all + both_x - both_w
    even_yz = diagonal_all - 2.0 * both_x
    cxy, cyx = bx + mx, by - my
    cxz, czx = bx - mx, bz + mz
    cyz, czy = by + my, bz - mz
    change = [12.0 * g_eps - 30.0 * g_e]

    def pair(even, odd_part):
        change.append(even + odd_part)
        change.append(even - odd_part)

    pair(even_x, ax)
    pair(even_y, ay)
    pair(even_z, az)
    pair(even_xy + g_pxy, cxy + cyx)
    pair(even_xy - g_pxy, cxy - cyx)
    pair(even_xz + g_pxz, cxz + czx)
    pair(even_xz - g_pxz, cxz - czx)
    pair(even_yz + g_pyz, cyz + czy)
    pair(even_yz - g_pyz, cyz - czy)
    return [jnp.where(solid, f[opposite[i]], f[i] + change[i]) for i in range(19)]


def kernel(
    sizes,
    scatter_hbm, speed_hbm, bubble_hbm, wall_hbm,
    fields_out,
    scatter, speed, bubble, wall,
    in_send, in_recv, out_send,
    edge_send, edge_x, edge_rest,
    pops, psi, solids,
    send, recv,
    load_sem, own_sem, in_sems, out_sems, edge_sems, round_sems,
):
    nx, ny, nz = sizes
    gx, gy, gz = lax.axis_index("gx"), lax.axis_index("gy"), lax.axis_index("gz")
    planes, groups = nx * 4, ny * 2
    X = gx * 4 + lax.div(gz, 2)
    Y = gy * 2 + lax.rem(gz, 2)

    def neighbour(e):
        x, y = lax.rem(X + (e[0] + planes), planes), lax.rem(Y + (e[1] + groups), groups)
        return {
            "gx": lax.div(x, 4),
            "gy": lax.div(y, 2),
            "gz": lax.rem(x, 4) * 2 + lax.rem(y, 2),
        }

    loads = [
        pltpu.make_async_copy(src, dst, load_sem.at[k])
        for k, (src, dst) in enumerate(
            ((scatter_hbm, scatter), (speed_hbm, speed), (bubble_hbm, bubble), (wall_hbm, wall))
        )
    ]
    for load in loads:
        load.start()
    barrier = pltpu.get_barrier_semaphore()
    where_to = [neighbour(e) for e in offsets + far]
    peers = [lax.rem(gz + k, nz) for k in range(1, nz)]
    for target in where_to[: len(offsets)] + [{"gx": gx, "gy": gy, "gz": peer} for peer in peers]:
        pl.semaphore_signal(barrier, inc=1, device_id=target, device_id_type=MESH)
    for load in loads:
        load.wait()

    for p in range(4):
        rho0 = jnp.where(bubble[p] == 1, 0.06, 0.28) * scatter[p]
        solid = jnp.where(wall[p] == 1, 1.0, 0.0)
        fields = [rho0, speed[0, p], speed[1, p], speed[2, p], solid]
        for half in range(2):
            first = (p * 2 + half) * IN_ROWS
            for k, field in enumerate(fields):
                in_send[first + k * ROWS : first + (k + 1) * ROWS, :] = field[half * ROWS : (half + 1) * ROWS]
    pl.semaphore_wait(barrier, len(offsets) + len(peers))

    def exchange(source, target, rows, sems):
        mine = pl.ds(pl.multiple_of(gz * rows, 8), rows)
        copies = []
        for k, peer in enumerate(peers):
            copy = pltpu.make_async_remote_copy(
                src_ref=source.at[pl.ds(pl.multiple_of(peer * rows, 8), rows), :],
                dst_ref=target.at[mine, :],
                send_sem=sems.at[0, k],
                recv_sem=sems.at[1, k],
                device_id={"gx": gx, "gy": gy, "gz": peer},
                device_id_type=MESH,
            )
            copy.start()
            copies.append(copy)
        own = pltpu.make_async_copy(source.at[mine, :], target.at[mine, :], own_sem)
        own.start()
        for copy in copies:
            copy.wait()
        own.wait()

    exchange(in_send, in_recv, IN_ROWS, in_sems)

    def line(field, c):
        return in_recv[pl.ds(field * ROWS + c, 8, stride=IN_ROWS), :]

    for c in range(ROWS):
        solid = line(4, c)
        solids[1, c + 1] = solid
        edge_send[c, 0] = jnp.where(solid > 0.5, 0.5, pseudo_potential(line(0, c)))
        edge_send[c, 1] = solid
    copies = []
    for k, e in reversed(list(enumerate(offsets))):
        if e[1] == 0:
            source, target = edge_send, edge_x.at[k]
        else:
            source, target = edge_send.at[ROWS - 1 if e[1] > 0 else 0], edge_rest.at[k - 2]
        copies.append(
            pltpu.make_async_remote_copy(
                src_ref=source,
                dst_ref=target,
                send_sem=edge_sems.at[0, k],
                recv_sem=edge_sems.at[1, k],
                device_id=where_to[k],
                device_id_type=MESH,
            )
        )
        copies[-1].start()
    for c in range(ROWS):
        for i, value in enumerate(equilibrium(line(0, c), (line(1, c), line(2, c), line(3, c)))):
            pops[0, i, c] = value
    for copy in copies:
        copy.wait()
    for k, e in enumerate(offsets):
        if e[1] == 0:
            for c in range(ROWS):
                psi[1 - e[0], c + 1] = edge_x[k, c, 0]
                solids[1 - e[0], c + 1] = edge_x[k, c, 1]
        else:
            y = 0 if e[1] > 0 else ROWS + 1
            psi[1 - e[0], y] = edge_rest[k - 2, 0]
            solids[1 - e[0], y] = edge_rest[k - 2, 1]

    lane = lax.broadcasted_iota(jnp.int32, (8, 128), 1)
    is_first, is_last = lane == 0, lane == 127

    def shift(v, by):
        rolled = pltpu.roll(v, 1 if by > 0 else 127, 1)
        carried = pltpu.roll(rolled, 1 if by > 0 else 7, 0)
        return jnp.where(is_first if by > 0 else is_last, carried, rolled)

    halo = [(x, y) for x in (-1, 0, 1) for y in range(-1, ROWS + 1) if in_halo(x, y, (0, 0))]

    def at(x, y):
        return psi[x + 1, y + 1]

    def potential_of(x, y, rho):
        psi[x + 1, y + 1] = jnp.where(solids[x + 1, y + 1] > 0.5, 0.5, pseudo_potential(rho))

    def step(r, now, later, last):
        for c in range(ROWS):
            potential_of(0, c, density_and_momentum([pops[now, i, c] for i in range(19)])[0])
        copies = []

        def launch(e, k, first, count):
            part = pl.ds(first, count)
            copies.append(
                pltpu.make_async_remote_copy(
                    src_ref=send.at[r, part],
                    dst_ref=recv.at[r, part],
                    send_sem=round_sems.at[0, r, k],
                    recv_sem=round_sems.at[1, r, k],
                    device_id=where_to[(offsets + far).index(e)],
                    device_id_type=MESH,
                )
            )
            copies[-1].start()

        share = {}
        for c in range(ROWS):
            here = at(0, c)
            spread = [at(1, y) - at(-1, y) for y in (c - 1, c, c + 1)]
            left, middle, right = [at(x, c + 1) - at(x, c - 1) for x in (-1, 0, 1)]
            around = 2.0 * here + ((at(-1, c) + at(1, c)) + (at(0, c - 1) + at(0, c + 1)))
            scale = here * (1.0 / 36.0)
            force = (
                scale * ((2.0 * spread[1] + (spread[0] + spread[2])) + (shift(spread[1], 1) + shift(spread[1], -1))),
                scale * ((2.0 * middle + (left + right)) + (shift(middle, 1) + shift(middle, -1))),
                scale * (shift(around, -1) - shift(around, 1)),
            )
            post = collide([pops[now, i, c] for i in range(19)], force, solids[1, c + 1] > 0.5)
            for i, (cx, cy, cz) in enumerate(velocities):
                value = shift(post[i], cz) if cz else post[i]
                node = cx, c + cy
                if not last:
                    share[node] = share[node] + value if node in share else value
                if in_block(*node, (0, 0)):
                    pops[later, i, c + cy] = value
                else:
                    for e in offsets:
                        if in_block(*node, e):
                            send[r, start_of[e] + pops_of[e].index((i, c))] = value
        for k, e in reversed(list(enumerate(offsets if last else offsets + far))):
            first, count = start_of[e], len(pops_of[e])
            if not last:
                for n, node in enumerate(shares_of[e]):
                    send[r, start_of[e] + len(pops_of[e]) + n] = share[node]
                count += len(shares_of[e])
            launch(e, k, first, count)
        for copy in copies:
            copy.wait()
        for e in offsets:
            for k, (i, c) in enumerate(pops_of[e]):
                pops[later, i, c + velocities[i][1] - ROWS * e[1]] = recv[r, start_of[e] + k]
        if not last:
            for x, y in halo:
                rho = share[x, y]
                for e in offsets + far:
                    there = (x + e[0], y + ROWS * e[1])
                    if there in shares_of[e]:
                        rho = rho + recv[r, start_of[e] + len(pops_of[e]) + shares_of[e].index(there)]
                potential_of(x, y, rho)

    def body(r, carry):
        now = lax.rem(r, 2)
        step(r, now, 1 - now, False)
        return carry

    lax.fori_loop(0, STEPS - 1, body, 0)
    step(STEPS - 1, (STEPS - 1) % 2, STEPS % 2, True)

    for c in range(ROWS):
        rho, momentum = density_and_momentum([pops[STEPS % 2, i, c] for i in range(19)])
        fluid = solids[1, c + 1] < 0.5
        scale = math.sqrt(3.0) / rho
        fields = [rho * (1.0 / 0.28)] + [j * scale for j in momentum]
        for k, field in enumerate(fields):
            out_send[pl.ds(k * ROWS + c, 8, stride=OUT_ROWS), :] = jnp.where(fluid, field, 0.0)
    exchange(out_send, fields_out, OUT_ROWS, out_sems)


def unpack(fields, density_out, velocity_out):
    for p in range(4):
        for half in range(2):
            first = (p * 2 + half) * OUT_ROWS
            rows = slice(half * ROWS, (half + 1) * ROWS)
            density_out[p, rows, :] = fields[first : first + ROWS, :]
            for k in range(3):
                velocity_out[k, p, rows, :] = fields[first + (k + 1) * ROWS : first + (k + 2) * ROWS, :]


def solution(mesh):
    sizes = (mesh.shape["gx"], mesh.shape["gy"], mesh.shape["gz"])
    block = (4, 8, 128)
    tile = (8, 128)

    def on_device(density_scatter, initial_velocity, bubble_mask, wall_flags):
        fields = pl.pallas_call(
                functools.partial(kernel, sizes),
                out_shape=jax.ShapeDtypeStruct((8 * OUT_ROWS, 128), jnp.float32),
                in_specs=[pl.BlockSpec(memory_space=pl.ANY)] * 4,
                out_specs=pl.BlockSpec(memory_space=pl.ANY),
                scratch_shapes=[
                    pltpu.VMEM(block, jnp.float32),
                    pltpu.VMEM((3,) + block, jnp.float32),
                    pltpu.VMEM(block, jnp.int32),
                    pltpu.VMEM(block, jnp.int32),
                    pltpu.VMEM((8 * IN_ROWS, 128), jnp.float32),
                    pltpu.VMEM((8 * IN_ROWS, 128), jnp.float32),
                    pltpu.VMEM((8 * OUT_ROWS, 128), jnp.float32),
                    pltpu.VMEM((ROWS, 2) + tile, jnp.float32),
                    pltpu.VMEM((2, ROWS, 2) + tile, jnp.float32),
                    pltpu.VMEM((6, 2) + tile, jnp.float32),
                    pltpu.VMEM((2, 19, ROWS) + tile, jnp.float32),
                    pltpu.VMEM((3, ROWS + 2) + tile, jnp.float32),
                    pltpu.VMEM((3, ROWS + 2) + tile, jnp.float32),
                    pltpu.VMEM((STEPS, TOTAL) + tile, jnp.float32),
                    pltpu.VMEM((STEPS, TOTAL) + tile, jnp.float32),
                    pltpu.SemaphoreType.DMA((4,)),
                    pltpu.SemaphoreType.DMA,
                    pltpu.SemaphoreType.DMA((2, 7)),
                    pltpu.SemaphoreType.DMA((2, 7)),
                    pltpu.SemaphoreType.DMA((2, 8)),
                    pltpu.SemaphoreType.DMA((2, STEPS, 14)),
                ],
                compiler_params=pltpu.CompilerParams(collective_id=0, has_side_effects=True),
            )(density_scatter, initial_velocity, bubble_mask, wall_flags)
        return tuple(
            pl.pallas_call(
                unpack,
                out_shape=[
                    jax.ShapeDtypeStruct(block, jnp.float32),
                    jax.ShapeDtypeStruct((3,) + block, jnp.float32),
                ],
                in_specs=[pl.BlockSpec(memory_space=pltpu.VMEM)],
                out_specs=[pl.BlockSpec(memory_space=pltpu.VMEM)] * 2,
            )(fields)
        )

    return jax.shard_map(
        on_device,
        mesh=mesh,
        in_specs=(
            P("gx", "gy", "gz"),
            P(None, "gx", "gy", "gz"),
            P("gx", "gy", "gz"),
            P("gx", "gy", "gz"),
        ),
        out_specs=(P("gx", "gy", "gz"), P(None, "gx", "gy", "gz")),
        check_vma=False,
    )
```

```python
import functools
import math

import jax
import jax.numpy as jnp
from jax import lax
from jax.experimental import pallas as pl
from jax.experimental.pallas import tpu as pltpu
from jax.sharding import PartitionSpec as P

STEPS = 4
MESH = pl.DeviceIdType.MESH
velocities = [
    (0, 0, 0),
    (1, 0, 0), (-1, 0, 0), (0, 1, 0), (0, -1, 0), (0, 0, 1), (0, 0, -1),
    (1, 1, 0), (-1, -1, 0), (1, -1, 0), (-1, 1, 0),
    (1, 0, 1), (-1, 0, -1), (1, 0, -1), (-1, 0, 1),
    (0, 1, 1), (0, -1, -1), (0, 1, -1), (0, -1, 1),
]
opposite = [0, 2, 1, 4, 3, 6, 5, 8, 7, 10, 9, 12, 11, 14, 13, 16, 15, 18, 17]
ROWS = 4
FIRST_ROWS = 8
NEXT_ROWS = 16
OUT_ROWS = 16

offsets = [(1, 0), (-1, 0), (0, 1), (0, -1), (1, 1), (1, -1), (-1, 1), (-1, -1)]
far = [(2, 1), (2, -1), (-2, 1), (-2, -1), (2, 0), (-2, 0)]


def in_block(x, y, e):
    return x == e[0] and ROWS * e[1] <= y < ROWS * e[1] + ROWS


def in_halo(x, y, e):
    near = abs(x - e[0]) <= 1 and ROWS * e[1] - 1 <= y <= ROWS * e[1] + ROWS
    return near and not in_block(x, y, e)


pops_of = {
    e: [
        (i, c)
        for c in range(ROWS)
        for i in range(19)
        if in_block(velocities[i][0], c + velocities[i][1], e)
    ]
    for e in offsets + far
}
shares_of = {
    e: [(x, y) for x in (-1, 0, 1) for y in range(-1, ROWS + 1) if in_halo(x, y, e)]
    for e in offsets + far
}
start_of, total = {}, 0
for e in offsets + far:
    start_of[e] = total
    total += len(pops_of[e]) + len(shares_of[e])
TOTAL = total


def pseudo_potential(rho):
    gap = 1.0 - rho
    square = rho * rho
    pressure = rho * 0.06 * (1.0 + rho + square - square * rho) / (gap * gap * gap) - square
    return jnp.sqrt(6.0 * (rho * (1.0 / 3.0) - pressure))


def equilibrium(rho, u):
    ux, uy, uz = u
    base = 1.0 - 1.5 * (ux * ux + uy * uy + uz * uz)
    third, axis, diagonal = rho * (1.0 / 3.0), rho * (1.0 / 18.0), rho * (1.0 / 36.0)
    out = [third * base]

    def pair(weight, projection):
        even = base + 4.5 * projection * projection
        odd = 3.0 * projection
        out.append(weight * (even + odd))
        out.append(weight * (even - odd))

    for value in (ux, uy, uz):
        pair(axis, value)
    for a, b in ((ux, uy), (ux, uz), (uy, uz)):
        pair(diagonal, a + b)
        pair(diagonal, a - b)
    return out


def density_and_momentum(f):
    s = {k: f[k] + f[k + 1] for k in range(1, 19, 2)}
    d = {k: f[k] - f[k + 1] for k in range(1, 19, 2)}
    rho = f[0] + (s[1] + s[3] + s[5]) + ((s[7] + s[9]) + (s[11] + s[13]) + (s[15] + s[17]))
    jx = d[1] + (d[7] + d[9]) + (d[11] + d[13])
    jy = d[3] + (d[7] - d[9]) + (d[15] + d[17])
    jz = d[5] + (d[11] - d[13]) + (d[15] - d[17])
    return rho, (jx, jy, jz)


def collide(f, force_over, solid):
    s = {k: f[k] + f[k + 1] for k in range(1, 19, 2)}
    d = {k: f[k] - f[k + 1] for k in range(1, 19, 2)}
    sx, sy, sz = s[1], s[3], s[5]
    sxy, sxz, syz = s[7] + s[9], s[11] + s[13], s[15] + s[17]
    pxy, pxz, pyz = s[7] - s[9], s[11] - s[13], s[15] - s[17]
    xy_x, xy_y = d[7] + d[9], d[7] - d[9]
    xz_x, xz_z = d[11] + d[13], d[11] - d[13]
    yz_y, yz_z = d[15] + d[17], d[15] - d[17]
    axes, diagonals = sx + sy + sz, sxy + sxz + syz
    rho = f[0] + axes + diagonals
    tx, ty, tz = xy_x + xz_x, xy_y + yz_y, xz_z + yz_z
    jx, jy, jz = d[1] + tx, d[3] + ty, d[5] + tz
    inverse = 1.0 / rho
    fx, fy, fz = force_over
    ux, uy, uz = jx * inverse, jy * inverse, jz * inverse
    vx, vy, vz = ux + fx * inverse, uy + fy * inverse, uz + fz * inverse
    exx, eyy, ezz = jx * ux, jy * uy, jz * uz
    exy, exz, eyz = jx * uy, jx * uz, jy * uz
    wx, wy, wz = rho * vx, rho * vy, rho * vz
    dxx, dyy, dzz = wx * vx - exx, wy * vy - eyy, wz * vz - ezz
    dxy, dxz, dyz = wx * vy - exy, wx * vz - exz, wy * vz - eyz
    e2, d2 = exx + eyy + ezz, dxx + dyy + dzz
    g_e = (1.19 * (-11.0 * rho + 19.0 * e2 - (-30.0 * f[0] - 11.0 * axes + 8.0 * diagonals)) + 19.0 * d2) * (1.0 / 2394.0)
    g_eps = (1.4 * (3.0 * rho - 5.5 * e2 - (12.0 * f[0] - 4.0 * axes + diagonals)) - 5.5 * d2) * (1.0 / 252.0)
    pxx_a, pxx_d = 3.0 * sx - axes, diagonals - 3.0 * syz
    pww_a, pww_d = sy - sz, sxy - sxz
    exx_e, dxx_e = 3.0 * exx - e2, 3.0 * dxx - d2
    eww_e, dww_e = eyy - ezz, dyy - dzz
    g_pxx = (1.25 * (exx_e - (pxx_a + pxx_d)) + dxx_e) * (1.0 / 36.0)
    g_pixx = (1.4 * (2.0 * pxx_a - pxx_d - 0.5 * exx_e) - 0.5 * dxx_e) * (1.0 / 72.0)
    g_pww = (1.25 * (eww_e - (pww_a + pww_d)) + dww_e) * (1.0 / 12.0)
    g_piww = (1.4 * (2.0 * pww_a - pww_d - 0.5 * eww_e) - 0.5 * dww_e) * (1.0 / 24.0)
    g_pxy = (1.25 * (exy - pxy) + dxy) * 0.25
    g_pxz = (1.25 * (exz - pxz) + dxz) * 0.25
    g_pyz = (1.25 * (eyz - pyz) + dyz) * 0.25

    def odd(j, axis, t, push):
        g_q = (1.2 * ((-2.0 / 3.0) * j + 4.0 * axis - t) - (2.0 / 3.0) * push) * (1.0 / 40.0)
        g_j = push * 0.1
        return g_j - 4.0 * g_q, g_j + g_q

    ax, bx = odd(jx, d[1], tx, fx)
    ay, by = odd(jy, d[3], ty, fy)
    az, bz = odd(jz, d[5], tz, fz)
    m = -1.98 / 8.0
    mx, my, mz = m * (xy_x - xz_x), m * (yz_y - xy_y), m * (xz_z - yz_z)
    axis_all = -11.0 * g_e - 4.0 * g_eps
    diagonal_all = 8.0 * g_e + g_eps
    part_x = g_pxx - 2.0 * g_pixx
    part_w = g_pww - 2.0 * g_piww
    even_x = axis_all + 2.0 * part_x
    even_y = axis_all - part_x + part_w
    even_z = axis_all - part_x - part_w
    both_x, both_w = g_pxx + g_pixx, g_pww + g_piww
    even_xy = diagonal_all + both_x + both_w
    even_xz = diagonal_all + both_x - both_w
    even_yz = diagonal_all - 2.0 * both_x
    cxy, cyx = bx + mx, by - my
    cxz, czx = bx - mx, bz + mz
    cyz, czy = by + my, bz - mz
    change = [12.0 * g_eps - 30.0 * g_e]

    def pair(even, odd_part):
        change.append(even + odd_part)
        change.append(even - odd_part)

    pair(even_x, ax)
    pair(even_y, ay)
    pair(even_z, az)
    pair(even_xy + g_pxy, cxy + cyx)
    pair(even_xy - g_pxy, cxy - cyx)
    pair(even_xz + g_pxz, cxz + czx)
    pair(even_xz - g_pxz, cxz - czx)
    pair(even_yz + g_pyz, cyz + czy)
    pair(even_yz - g_pyz, cyz - czy)
    return [jnp.where(solid, f[opposite[i]], f[i] + change[i]) for i in range(19)]


def kernel(
    sizes,
    scatter_hbm, speed_hbm, bubble_hbm, wall_hbm,
    fields_out,
    scatter, speed, bubble, wall,
    first_send, first_recv, next_send, next_recv, out_send,
    edge_send, edge_x, edge_rest,
    pops, psi, solids,
    send, recv,
    load_sem, own_sem, in_sems, out_sems, edge_sems, round_sems,
):
    nx, ny, nz = sizes
    gx, gy, gz = lax.axis_index("gx"), lax.axis_index("gy"), lax.axis_index("gz")
    planes, groups = nx * 4, ny * 2
    X = gx * 4 + lax.div(gz, 2)
    Y = gy * 2 + lax.rem(gz, 2)

    def neighbour(e):
        x, y = lax.rem(X + (e[0] + planes), planes), lax.rem(Y + (e[1] + groups), groups)
        return {
            "gx": lax.div(x, 4),
            "gy": lax.div(y, 2),
            "gz": lax.rem(x, 4) * 2 + lax.rem(y, 2),
        }

    loads = [
        pltpu.make_async_copy(src, dst, load_sem.at[k])
        for k, (src, dst) in enumerate(
            ((scatter_hbm, scatter), (speed_hbm, speed), (bubble_hbm, bubble), (wall_hbm, wall))
        )
    ]
    for load in loads:
        load.start()
    barrier = pltpu.get_barrier_semaphore()
    where_to = [neighbour(e) for e in offsets + far]
    bits = [lax.rem(gz, 2), lax.rem(lax.div(gz, 2), 2), lax.div(gz, 4)]
    peers = [
        sum((1 - bit if k & (1 << n) else bit) * (1 << n) for n, bit in enumerate(bits))
        for k in range(7, 0, -1)
    ]
    for target in where_to[: len(offsets)] + [{"gx": gx, "gy": gy, "gz": peer} for peer in peers]:
        pl.semaphore_signal(barrier, inc=1, device_id=target, device_id_type=MESH)
    for load in loads:
        load.wait()

    for p in range(4):
        rho0 = jnp.where(bubble[p] == 1, 0.06, 0.28) * scatter[p]
        solid = jnp.where(wall[p] == 1, 1.0, 0.0)
        for half in range(2):
            rows = slice(half * ROWS, (half + 1) * ROWS)
            for packed, size, group in (
                (first_send, FIRST_ROWS, (rho0, solid)),
                (next_send, NEXT_ROWS, (speed[0, p], speed[1, p], speed[2, p])),
            ):
                first = (p * 2 + half) * size
                for k, field in enumerate(group):
                    packed[first + k * ROWS : first + (k + 1) * ROWS, :] = field[rows]
    pl.semaphore_wait(barrier, len(offsets) + len(peers))

    def exchange(source, target, rows, sems, own_sem):
        mine = pl.ds(pl.multiple_of(gz * rows, 8), rows)
        copies = []
        for k, peer in enumerate(peers):
            copies.append(
                pltpu.make_async_remote_copy(
                    src_ref=source.at[pl.ds(pl.multiple_of(peer * rows, 8), rows), :],
                    dst_ref=target.at[mine, :],
                    send_sem=sems.at[0, k],
                    recv_sem=sems.at[1, k],
                    device_id={"gx": gx, "gy": gy, "gz": peer},
                    device_id_type=MESH,
                )
            )
            copies[-1].start()
        copies.append(pltpu.make_async_copy(source.at[mine, :], target.at[mine, :], own_sem))
        copies[-1].start()
        return copies

    first_copies = exchange(first_send, first_recv, FIRST_ROWS, in_sems.at[0], own_sem.at[0])
    next_copies = exchange(next_send, next_recv, NEXT_ROWS, in_sems.at[1], own_sem.at[1])
    for copy in first_copies:
        copy.wait()

    def line(packed, rows, field, c):
        return packed[pl.ds(field * ROWS + c, 8, stride=rows), :]

    for c in range(ROWS):
        solid = line(first_recv, FIRST_ROWS, 1, c)
        rho0 = line(first_recv, FIRST_ROWS, 0, c)
        solids[1, c + 1] = solid
        edge_send[c, 0] = jnp.where(solid > 0.5, 0.5, pseudo_potential(rho0))
        edge_send[c, 1] = solid
    copies = []
    for k, e in reversed(list(enumerate(offsets))):
        if e[1] == 0:
            source, target = edge_send, edge_x.at[k]
        else:
            source, target = edge_send.at[ROWS - 1 if e[1] > 0 else 0], edge_rest.at[k - 2]
        copies.append(
            pltpu.make_async_remote_copy(
                src_ref=source,
                dst_ref=target,
                send_sem=edge_sems.at[0, k],
                recv_sem=edge_sems.at[1, k],
                device_id=where_to[k],
                device_id_type=MESH,
            )
        )
        copies[-1].start()
    for copy in next_copies:
        copy.wait()
    for c in range(ROWS):
        rho0 = line(first_recv, FIRST_ROWS, 0, c)
        speed0 = [line(next_recv, NEXT_ROWS, k, c) for k in range(3)]
        for i, value in enumerate(equilibrium(rho0, speed0)):
            pops[0, i, c] = value
    for copy in copies:
        copy.wait()
    for k, e in enumerate(offsets):
        if e[1] == 0:
            for c in range(ROWS):
                psi[1 - e[0], c + 1] = edge_x[k, c, 0]
                solids[1 - e[0], c + 1] = edge_x[k, c, 1]
        else:
            y = 0 if e[1] > 0 else ROWS + 1
            psi[1 - e[0], y] = edge_rest[k - 2, 0]
            solids[1 - e[0], y] = edge_rest[k - 2, 1]

    lane = lax.broadcasted_iota(jnp.int32, (8, 128), 1)
    is_first, is_last = lane == 0, lane == 127

    def shift(v, by):
        rolled = pltpu.roll(v, 1 if by > 0 else 127, 1)
        carried = pltpu.roll(rolled, 1 if by > 0 else 7, 0)
        return jnp.where(is_first if by > 0 else is_last, carried, rolled)

    halo = [(x, y) for x in (-1, 0, 1) for y in range(-1, ROWS + 1) if in_halo(x, y, (0, 0))]

    def at(x, y):
        return psi[x + 1, y + 1]

    def potential_of(x, y, rho):
        psi[x + 1, y + 1] = jnp.where(solids[x + 1, y + 1] > 0.5, 0.5, pseudo_potential(rho))

    def step(r, now, later, last):
        for c in range(ROWS):
            potential_of(0, c, density_and_momentum([pops[now, i, c] for i in range(19)])[0])
        copies = []

        def launch(e, k, first, count):
            part = pl.ds(first, count)
            copies.append(
                pltpu.make_async_remote_copy(
                    src_ref=send.at[r, part],
                    dst_ref=recv.at[r, part],
                    send_sem=round_sems.at[0, r, k],
                    recv_sem=round_sems.at[1, r, k],
                    device_id=where_to[(offsets + far).index(e)],
                    device_id_type=MESH,
                )
            )
            copies[-1].start()

        share = {}
        for c in range(ROWS):
            here = at(0, c)
            spread = [at(1, y) - at(-1, y) for y in (c - 1, c, c + 1)]
            left, middle, right = [at(x, c + 1) - at(x, c - 1) for x in (-1, 0, 1)]
            around = 2.0 * here + ((at(-1, c) + at(1, c)) + (at(0, c - 1) + at(0, c + 1)))
            scale = here * (1.0 / 36.0)
            force = (
                scale * ((2.0 * spread[1] + (spread[0] + spread[2])) + (shift(spread[1], 1) + shift(spread[1], -1))),
                scale * ((2.0 * middle + (left + right)) + (shift(middle, 1) + shift(middle, -1))),
                scale * (shift(around, -1) - shift(around, 1)),
            )
            post = collide([pops[now, i, c] for i in range(19)], force, solids[1, c + 1] > 0.5)
            for i, (cx, cy, cz) in enumerate(velocities):
                value = shift(post[i], cz) if cz else post[i]
                node = cx, c + cy
                if not last:
                    share[node] = share[node] + value if node in share else value
                if in_block(*node, (0, 0)):
                    pops[later, i, c + cy] = value
                else:
                    for e in offsets:
                        if in_block(*node, e):
                            send[r, start_of[e] + pops_of[e].index((i, c))] = value
        for k, e in reversed(list(enumerate(offsets if last else offsets + far))):
            first, count = start_of[e], len(pops_of[e])
            if not last:
                for n, node in enumerate(shares_of[e]):
                    send[r, start_of[e] + len(pops_of[e]) + n] = share[node]
                count += len(shares_of[e])
            launch(e, k, first, count)
        for copy in copies:
            copy.wait()
        for e in offsets:
            for k, (i, c) in enumerate(pops_of[e]):
                pops[later, i, c + velocities[i][1] - ROWS * e[1]] = recv[r, start_of[e] + k]
        if not last:
            for x, y in halo:
                rho = share[x, y]
                for e in offsets + far:
                    there = (x + e[0], y + ROWS * e[1])
                    if there in shares_of[e]:
                        rho = rho + recv[r, start_of[e] + len(pops_of[e]) + shares_of[e].index(there)]
                potential_of(x, y, rho)

    def body(r, carry):
        now = lax.rem(r, 2)
        step(r, now, 1 - now, False)
        return carry

    lax.fori_loop(0, STEPS - 1, body, 0)
    step(STEPS - 1, (STEPS - 1) % 2, STEPS % 2, True)

    for c in range(ROWS):
        rho, momentum = density_and_momentum([pops[STEPS % 2, i, c] for i in range(19)])
        fluid = solids[1, c + 1] < 0.5
        scale = math.sqrt(3.0) / rho
        fields = [rho * (1.0 / 0.28)] + [j * scale for j in momentum]
        for k, field in enumerate(fields):
            out_send[pl.ds(k * ROWS + c, 8, stride=OUT_ROWS), :] = jnp.where(fluid, field, 0.0)
    for copy in exchange(out_send, fields_out, OUT_ROWS, out_sems, own_sem.at[2]):
        copy.wait()


def unpack(fields, density_out, velocity_out):
    for p in range(4):
        for half in range(2):
            first = (p * 2 + half) * OUT_ROWS
            rows = slice(half * ROWS, (half + 1) * ROWS)
            density_out[p, rows, :] = fields[first : first + ROWS, :]
            for k in range(3):
                velocity_out[k, p, rows, :] = fields[first + (k + 1) * ROWS : first + (k + 2) * ROWS, :]


def solution(mesh):
    sizes = (mesh.shape["gx"], mesh.shape["gy"], mesh.shape["gz"])
    block = (4, 8, 128)
    tile = (8, 128)

    def on_device(density_scatter, initial_velocity, bubble_mask, wall_flags):
        fields = pl.pallas_call(
                functools.partial(kernel, sizes),
                out_shape=jax.ShapeDtypeStruct((8 * OUT_ROWS, 128), jnp.float32),
                in_specs=[pl.BlockSpec(memory_space=pl.ANY)] * 4,
                out_specs=pl.BlockSpec(memory_space=pl.ANY),
                scratch_shapes=[
                    pltpu.VMEM(block, jnp.float32),
                    pltpu.VMEM((3,) + block, jnp.float32),
                    pltpu.VMEM(block, jnp.int32),
                    pltpu.VMEM(block, jnp.int32),
                    pltpu.VMEM((8 * FIRST_ROWS, 128), jnp.float32),
                    pltpu.VMEM((8 * FIRST_ROWS, 128), jnp.float32),
                    pltpu.VMEM((8 * NEXT_ROWS, 128), jnp.float32),
                    pltpu.VMEM((8 * NEXT_ROWS, 128), jnp.float32),
                    pltpu.VMEM((8 * OUT_ROWS, 128), jnp.float32),
                    pltpu.VMEM((ROWS, 2) + tile, jnp.float32),
                    pltpu.VMEM((2, ROWS, 2) + tile, jnp.float32),
                    pltpu.VMEM((6, 2) + tile, jnp.float32),
                    pltpu.VMEM((2, 19, ROWS) + tile, jnp.float32),
                    pltpu.VMEM((3, ROWS + 2) + tile, jnp.float32),
                    pltpu.VMEM((3, ROWS + 2) + tile, jnp.float32),
                    pltpu.VMEM((STEPS, TOTAL) + tile, jnp.float32),
                    pltpu.VMEM((STEPS, TOTAL) + tile, jnp.float32),
                    pltpu.SemaphoreType.DMA((4,)),
                    pltpu.SemaphoreType.DMA((3,)),
                    pltpu.SemaphoreType.DMA((2, 2, 7)),
                    pltpu.SemaphoreType.DMA((2, 7)),
                    pltpu.SemaphoreType.DMA((2, 8)),
                    pltpu.SemaphoreType.DMA((2, STEPS, 14)),
                ],
                compiler_params=pltpu.CompilerParams(collective_id=0, has_side_effects=True),
            )(density_scatter, initial_velocity, bubble_mask, wall_flags)
        return tuple(
            pl.pallas_call(
                unpack,
                out_shape=[
                    jax.ShapeDtypeStruct(block, jnp.float32),
                    jax.ShapeDtypeStruct((3,) + block, jnp.float32),
                ],
                in_specs=[pl.BlockSpec(memory_space=pltpu.VMEM)],
                out_specs=[pl.BlockSpec(memory_space=pltpu.VMEM)] * 2,
            )(fields)
        )

    return jax.shard_map(
        on_device,
        mesh=mesh,
        in_specs=(
            P("gx", "gy", "gz"),
            P(None, "gx", "gy", "gz"),
            P("gx", "gy", "gz"),
            P("gx", "gy", "gz"),
        ),
        out_specs=(P("gx", "gy", "gz"), P(None, "gx", "gy", "gz")),
        check_vma=False,
    )
```

```python
import functools
import math

import jax
import jax.numpy as jnp
from jax import lax
from jax.experimental import pallas as pl
from jax.experimental.pallas import tpu as pltpu
from jax.sharding import PartitionSpec as P

STEPS = 4
MESH = pl.DeviceIdType.MESH
velocities = [
    (0, 0, 0),
    (1, 0, 0), (-1, 0, 0), (0, 1, 0), (0, -1, 0), (0, 0, 1), (0, 0, -1),
    (1, 1, 0), (-1, -1, 0), (1, -1, 0), (-1, 1, 0),
    (1, 0, 1), (-1, 0, -1), (1, 0, -1), (-1, 0, 1),
    (0, 1, 1), (0, -1, -1), (0, 1, -1), (0, -1, 1),
]
opposite = [0, 2, 1, 4, 3, 6, 5, 8, 7, 10, 9, 12, 11, 14, 13, 16, 15, 18, 17]
ROWS = 4
FIRST_ROWS = 8
NEXT_ROWS = 16
OUT_ROWS = 16

offsets = [(1, 0), (-1, 0), (0, 1), (0, -1), (1, 1), (1, -1), (-1, 1), (-1, -1)]
far = [(2, 1), (2, -1), (-2, 1), (-2, -1), (2, 0), (-2, 0)]


def in_block(x, y, e):
    return x == e[0] and ROWS * e[1] <= y < ROWS * e[1] + ROWS


def in_halo(x, y, e):
    near = abs(x - e[0]) <= 1 and ROWS * e[1] - 1 <= y <= ROWS * e[1] + ROWS
    return near and not in_block(x, y, e)


pops_of = {
    e: [
        (i, c)
        for c in range(ROWS)
        for i in range(19)
        if in_block(velocities[i][0], c + velocities[i][1], e)
    ]
    for e in offsets + far
}
shares_of = {
    e: [(x, y) for x in (-1, 0, 1) for y in range(-1, ROWS + 1) if in_halo(x, y, e)]
    for e in offsets + far
}
start_of, total = {}, 0
for e in offsets + far:
    start_of[e] = total
    total += len(pops_of[e]) + len(shares_of[e])
TOTAL = total


def pseudo_potential(rho):
    gap = 1.0 - rho
    square = rho * rho
    pressure = rho * 0.06 * (1.0 + rho + square - square * rho) / (gap * gap * gap) - square
    return jnp.sqrt(6.0 * (rho * (1.0 / 3.0) - pressure))


def equilibrium(rho, u):
    ux, uy, uz = u
    base = 1.0 - 1.5 * (ux * ux + uy * uy + uz * uz)
    third, axis, diagonal = rho * (1.0 / 3.0), rho * (1.0 / 18.0), rho * (1.0 / 36.0)
    out = [third * base]

    def pair(weight, projection):
        even = base + 4.5 * projection * projection
        odd = 3.0 * projection
        out.append(weight * (even + odd))
        out.append(weight * (even - odd))

    for value in (ux, uy, uz):
        pair(axis, value)
    for a, b in ((ux, uy), (ux, uz), (uy, uz)):
        pair(diagonal, a + b)
        pair(diagonal, a - b)
    return out


def density_and_momentum(f):
    s = {k: f[k] + f[k + 1] for k in range(1, 19, 2)}
    d = {k: f[k] - f[k + 1] for k in range(1, 19, 2)}
    rho = f[0] + (s[1] + s[3] + s[5]) + ((s[7] + s[9]) + (s[11] + s[13]) + (s[15] + s[17]))
    jx = d[1] + (d[7] + d[9]) + (d[11] + d[13])
    jy = d[3] + (d[7] - d[9]) + (d[15] + d[17])
    jz = d[5] + (d[11] - d[13]) + (d[15] - d[17])
    return rho, (jx, jy, jz)


def collide(f, force_over, solid):
    s = {k: f[k] + f[k + 1] for k in range(1, 19, 2)}
    d = {k: f[k] - f[k + 1] for k in range(1, 19, 2)}
    sx, sy, sz = s[1], s[3], s[5]
    sxy, sxz, syz = s[7] + s[9], s[11] + s[13], s[15] + s[17]
    pxy, pxz, pyz = s[7] - s[9], s[11] - s[13], s[15] - s[17]
    xy_x, xy_y = d[7] + d[9], d[7] - d[9]
    xz_x, xz_z = d[11] + d[13], d[11] - d[13]
    yz_y, yz_z = d[15] + d[17], d[15] - d[17]
    axes, diagonals = sx + sy + sz, sxy + sxz + syz
    rho = f[0] + axes + diagonals
    tx, ty, tz = xy_x + xz_x, xy_y + yz_y, xz_z + yz_z
    jx, jy, jz = d[1] + tx, d[3] + ty, d[5] + tz
    inverse = 1.0 / rho
    fx, fy, fz = force_over
    ux, uy, uz = jx * inverse, jy * inverse, jz * inverse
    vx, vy, vz = ux + fx * inverse, uy + fy * inverse, uz + fz * inverse
    exx, eyy, ezz = jx * ux, jy * uy, jz * uz
    exy, exz, eyz = jx * uy, jx * uz, jy * uz
    wx, wy, wz = rho * vx, rho * vy, rho * vz
    dxx, dyy, dzz = wx * vx - exx, wy * vy - eyy, wz * vz - ezz
    dxy, dxz, dyz = wx * vy - exy, wx * vz - exz, wy * vz - eyz
    e2, d2 = exx + eyy + ezz, dxx + dyy + dzz
    g_e = (1.19 * (-11.0 * rho + 19.0 * e2 - (-30.0 * f[0] - 11.0 * axes + 8.0 * diagonals)) + 19.0 * d2) * (1.0 / 2394.0)
    g_eps = (1.4 * (3.0 * rho - 5.5 * e2 - (12.0 * f[0] - 4.0 * axes + diagonals)) - 5.5 * d2) * (1.0 / 252.0)
    pxx_a, pxx_d = 3.0 * sx - axes, diagonals - 3.0 * syz
    pww_a, pww_d = sy - sz, sxy - sxz
    exx_e, dxx_e = 3.0 * exx - e2, 3.0 * dxx - d2
    eww_e, dww_e = eyy - ezz, dyy - dzz
    g_pxx = (1.25 * (exx_e - (pxx_a + pxx_d)) + dxx_e) * (1.0 / 36.0)
    g_pixx = (1.4 * (2.0 * pxx_a - pxx_d - 0.5 * exx_e) - 0.5 * dxx_e) * (1.0 / 72.0)
    g_pww = (1.25 * (eww_e - (pww_a + pww_d)) + dww_e) * (1.0 / 12.0)
    g_piww = (1.4 * (2.0 * pww_a - pww_d - 0.5 * eww_e) - 0.5 * dww_e) * (1.0 / 24.0)
    g_pxy = (1.25 * (exy - pxy) + dxy) * 0.25
    g_pxz = (1.25 * (exz - pxz) + dxz) * 0.25
    g_pyz = (1.25 * (eyz - pyz) + dyz) * 0.25

    def odd(j, axis, t, push):
        g_q = (1.2 * ((-2.0 / 3.0) * j + 4.0 * axis - t) - (2.0 / 3.0) * push) * (1.0 / 40.0)
        g_j = push * 0.1
        return g_j - 4.0 * g_q, g_j + g_q

    ax, bx = odd(jx, d[1], tx, fx)
    ay, by = odd(jy, d[3], ty, fy)
    az, bz = odd(jz, d[5], tz, fz)
    m = -1.98 / 8.0
    mx, my, mz = m * (xy_x - xz_x), m * (yz_y - xy_y), m * (xz_z - yz_z)
    axis_all = -11.0 * g_e - 4.0 * g_eps
    diagonal_all = 8.0 * g_e + g_eps
    part_x = g_pxx - 2.0 * g_pixx
    part_w = g_pww - 2.0 * g_piww
    even_x = axis_all + 2.0 * part_x
    even_y = axis_all - part_x + part_w
    even_z = axis_all - part_x - part_w
    both_x, both_w = g_pxx + g_pixx, g_pww + g_piww
    even_xy = diagonal_all + both_x + both_w
    even_xz = diagonal_all + both_x - both_w
    even_yz = diagonal_all - 2.0 * both_x
    cxy, cyx = bx + mx, by - my
    cxz, czx = bx - mx, bz + mz
    cyz, czy = by + my, bz - mz
    change = [12.0 * g_eps - 30.0 * g_e]

    def pair(even, odd_part):
        change.append(even + odd_part)
        change.append(even - odd_part)

    pair(even_x, ax)
    pair(even_y, ay)
    pair(even_z, az)
    pair(even_xy + g_pxy, cxy + cyx)
    pair(even_xy - g_pxy, cxy - cyx)
    pair(even_xz + g_pxz, cxz + czx)
    pair(even_xz - g_pxz, cxz - czx)
    pair(even_yz + g_pyz, cyz + czy)
    pair(even_yz - g_pyz, cyz - czy)
    return [jnp.where(solid, f[opposite[i]], f[i] + change[i]) for i in range(19)]


def kernel(
    sizes,
    scatter_hbm, speed_hbm, bubble_hbm, wall_hbm,
    fields_out,
    scatter, speed, bubble, wall,
    first_send, first_recv, next_send, next_recv, out_send,
    edge_send, edge_x, edge_rest,
    pops, psi, solids,
    send, recv,
    load_sem, own_sem, in_sems, out_sems, edge_sems, round_sems,
):
    nx, ny, nz = sizes
    gx, gy, gz = lax.axis_index("gx"), lax.axis_index("gy"), lax.axis_index("gz")
    planes, groups = nx * 4, ny * 2
    X = gx * 4 + lax.div(gz, 2)
    Y = gy * 2 + lax.rem(gz, 2)

    def neighbour(e):
        x, y = lax.rem(X + (e[0] + planes), planes), lax.rem(Y + (e[1] + groups), groups)
        return {
            "gx": lax.div(x, 4),
            "gy": lax.div(y, 2),
            "gz": lax.rem(x, 4) * 2 + lax.rem(y, 2),
        }

    loads = [
        pltpu.make_async_copy(src, dst, load_sem.at[k])
        for k, (src, dst) in enumerate(
            ((scatter_hbm, scatter), (speed_hbm, speed), (bubble_hbm, bubble), (wall_hbm, wall))
        )
    ]
    for load in loads:
        load.start()
    barrier = pltpu.get_barrier_semaphore()
    where_to = [neighbour(e) for e in offsets + far]
    bits = [lax.rem(gz, 2), lax.rem(lax.div(gz, 2), 2), lax.div(gz, 4)]
    peers = [
        sum((1 - bit if k & (1 << n) else bit) * (1 << n) for n, bit in enumerate(bits))
        for k in range(7, 0, -1)
    ]
    for target in where_to[: len(offsets)] + [{"gx": gx, "gy": gy, "gz": peer} for peer in peers]:
        pl.semaphore_signal(barrier, inc=1, device_id=target, device_id_type=MESH)
    for load in loads:
        load.wait()

    for p in range(4):
        rho0 = jnp.where(bubble[p] == 1, 0.06, 0.28) * scatter[p]
        solid = jnp.where(wall[p] == 1, 1.0, 0.0)
        for half in range(2):
            rows = slice(half * ROWS, (half + 1) * ROWS)
            for packed, size, group in (
                (first_send, FIRST_ROWS, (rho0, solid)),
                (next_send, NEXT_ROWS, (speed[0, p], speed[1, p], speed[2, p])),
            ):
                first = (p * 2 + half) * size
                for k, field in enumerate(group):
                    packed[first + k * ROWS : first + (k + 1) * ROWS, :] = field[rows]
    pl.semaphore_wait(barrier, len(offsets) + len(peers))

    def exchange(source, target, rows, sems, own_sem):
        mine = pl.ds(pl.multiple_of(gz * rows, 8), rows)
        copies = []
        for k, peer in enumerate(peers):
            copies.append(
                pltpu.make_async_remote_copy(
                    src_ref=source.at[pl.ds(pl.multiple_of(peer * rows, 8), rows), :],
                    dst_ref=target.at[mine, :],
                    send_sem=sems.at[0, k],
                    recv_sem=sems.at[1, k],
                    device_id={"gx": gx, "gy": gy, "gz": peer},
                    device_id_type=MESH,
                )
            )
            copies[-1].start()
        copies.append(pltpu.make_async_copy(source.at[mine, :], target.at[mine, :], own_sem))
        copies[-1].start()
        return copies

    first_copies = exchange(first_send, first_recv, FIRST_ROWS, in_sems.at[0], own_sem.at[0])
    next_copies = exchange(next_send, next_recv, NEXT_ROWS, in_sems.at[1], own_sem.at[1])
    for copy in first_copies:
        copy.wait()

    def line(packed, rows, field, c):
        return packed[pl.ds(field * ROWS + c, 8, stride=rows), :]

    for c in range(ROWS):
        solid = line(first_recv, FIRST_ROWS, 1, c)
        rho0 = line(first_recv, FIRST_ROWS, 0, c)
        solids[1, c + 1] = solid
        edge_send[c, 0] = jnp.where(solid > 0.5, 0.5, pseudo_potential(rho0))
        edge_send[c, 1] = solid
    copies = []
    for k, e in reversed(list(enumerate(offsets))):
        if e[1] == 0:
            source, target = edge_send, edge_x.at[k]
        else:
            source, target = edge_send.at[ROWS - 1 if e[1] > 0 else 0], edge_rest.at[k - 2]
        copies.append(
            pltpu.make_async_remote_copy(
                src_ref=source,
                dst_ref=target,
                send_sem=edge_sems.at[0, k],
                recv_sem=edge_sems.at[1, k],
                device_id=where_to[k],
                device_id_type=MESH,
            )
        )
        copies[-1].start()
    for copy in next_copies:
        copy.wait()
    for c in range(ROWS):
        rho0 = line(first_recv, FIRST_ROWS, 0, c)
        speed0 = [line(next_recv, NEXT_ROWS, k, c) for k in range(3)]
        for i, value in enumerate(equilibrium(rho0, speed0)):
            pops[0, i, c] = value
    for copy in copies:
        copy.wait()
    for k, e in enumerate(offsets):
        if e[1] == 0:
            for c in range(ROWS):
                psi[1 - e[0], c + 1] = edge_x[k, c, 0]
                solids[1 - e[0], c + 1] = edge_x[k, c, 1]
        else:
            y = 0 if e[1] > 0 else ROWS + 1
            psi[1 - e[0], y] = edge_rest[k - 2, 0]
            solids[1 - e[0], y] = edge_rest[k - 2, 1]

    lane = lax.broadcasted_iota(jnp.int32, (8, 128), 1)
    is_first, is_last = lane == 0, lane == 127

    def shift(v, by):
        rolled = pltpu.roll(v, 1 if by > 0 else 127, 1)
        carried = pltpu.roll(rolled, 1 if by > 0 else 7, 0)
        return jnp.where(is_first if by > 0 else is_last, carried, rolled)

    halo = [(x, y) for x in (-1, 0, 1) for y in range(-1, ROWS + 1) if in_halo(x, y, (0, 0))]

    def at(x, y):
        return psi[x + 1, y + 1]

    def potential_of(x, y, rho):
        psi[x + 1, y + 1] = jnp.where(solids[x + 1, y + 1] > 0.5, 0.5, pseudo_potential(rho))

    def step(r, now, later, last):
        for c in range(ROWS):
            potential_of(0, c, density_and_momentum([pops[now, i, c] for i in range(19)])[0])
        copies = []

        def launch(e, k, first, count):
            part = pl.ds(first, count)
            copies.append(
                pltpu.make_async_remote_copy(
                    src_ref=send.at[r, part],
                    dst_ref=recv.at[r, part],
                    send_sem=round_sems.at[0, r, k],
                    recv_sem=round_sems.at[1, r, k],
                    device_id=where_to[(offsets + far).index(e)],
                    device_id_type=MESH,
                )
            )
            copies[-1].start()

        share = {}
        for c in range(ROWS):
            here = at(0, c)
            spread = [at(1, y) - at(-1, y) for y in (c - 1, c, c + 1)]
            left, middle, right = [at(x, c + 1) - at(x, c - 1) for x in (-1, 0, 1)]
            around = 2.0 * here + ((at(-1, c) + at(1, c)) + (at(0, c - 1) + at(0, c + 1)))
            scale = here * (1.0 / 36.0)
            force = (
                scale * ((2.0 * spread[1] + (spread[0] + spread[2])) + (shift(spread[1], 1) + shift(spread[1], -1))),
                scale * ((2.0 * middle + (left + right)) + (shift(middle, 1) + shift(middle, -1))),
                scale * (shift(around, -1) - shift(around, 1)),
            )
            post = collide([pops[now, i, c] for i in range(19)], force, solids[1, c + 1] > 0.5)
            for i, (cx, cy, cz) in enumerate(velocities):
                value = shift(post[i], cz) if cz else post[i]
                node = cx, c + cy
                if not last:
                    share[node] = share[node] + value if node in share else value
                if in_block(*node, (0, 0)):
                    pops[later, i, c + cy] = value
                else:
                    for e in offsets:
                        if in_block(*node, e):
                            send[r, start_of[e] + pops_of[e].index((i, c))] = value
        for k, e in reversed(list(enumerate(offsets if last else offsets + far))):
            first, count = start_of[e], len(pops_of[e])
            if not last:
                for n, node in enumerate(shares_of[e]):
                    send[r, start_of[e] + len(pops_of[e]) + n] = share[node]
                count += len(shares_of[e])
            launch(e, k, first, count)
        for copy in copies:
            copy.wait()
        for e in offsets:
            for k, (i, c) in enumerate(pops_of[e]):
                pops[later, i, c + velocities[i][1] - ROWS * e[1]] = recv[r, start_of[e] + k]
        if not last:
            for x, y in halo:
                rho = share[x, y]
                for e in offsets + far:
                    there = (x + e[0], y + ROWS * e[1])
                    if there in shares_of[e]:
                        rho = rho + recv[r, start_of[e] + len(pops_of[e]) + shares_of[e].index(there)]
                potential_of(x, y, rho)

    def body(r, carry):
        now = lax.rem(r, 2)
        step(r, now, 1 - now, False)
        return carry

    lax.fori_loop(0, STEPS - 1, body, 0)
    step(STEPS - 1, (STEPS - 1) % 2, STEPS % 2, True)

    for c in range(ROWS):
        rho, momentum = density_and_momentum([pops[STEPS % 2, i, c] for i in range(19)])
        fluid = solids[1, c + 1] < 0.5
        scale = math.sqrt(3.0) / rho
        fields = [rho * (1.0 / 0.28)] + [j * scale for j in momentum]
        for k, field in enumerate(fields):
            out_send[pl.ds(k * ROWS + c, 8, stride=OUT_ROWS), :] = jnp.where(fluid, field, 0.0)
    for copy in exchange(out_send, fields_out, OUT_ROWS, out_sems, own_sem.at[2]):
        copy.wait()


def unpack(fields, density_out, velocity_out):
    for p in range(4):
        for half in range(2):
            first = (p * 2 + half) * OUT_ROWS
            rows = slice(half * ROWS, (half + 1) * ROWS)
            density_out[p, rows, :] = fields[first : first + ROWS, :]
            for k in range(3):
                velocity_out[k, p, rows, :] = fields[first + (k + 1) * ROWS : first + (k + 2) * ROWS, :]


def solution(mesh):
    sizes = (mesh.shape["gx"], mesh.shape["gy"], mesh.shape["gz"])
    block = (4, 8, 128)
    tile = (8, 128)

    def on_device(density_scatter, initial_velocity, bubble_mask, wall_flags):
        fields = pl.pallas_call(
                functools.partial(kernel, sizes),
                out_shape=jax.ShapeDtypeStruct((8 * OUT_ROWS, 128), jnp.float32),
                in_specs=[pl.BlockSpec(memory_space=pltpu.HBM)] * 4,
                out_specs=pl.BlockSpec(memory_space=pltpu.VMEM),
                scratch_shapes=[
                    pltpu.VMEM(block, jnp.float32),
                    pltpu.VMEM((3,) + block, jnp.float32),
                    pltpu.VMEM(block, jnp.int32),
                    pltpu.VMEM(block, jnp.int32),
                    pltpu.VMEM((8 * FIRST_ROWS, 128), jnp.float32),
                    pltpu.VMEM((8 * FIRST_ROWS, 128), jnp.float32),
                    pltpu.VMEM((8 * NEXT_ROWS, 128), jnp.float32),
                    pltpu.VMEM((8 * NEXT_ROWS, 128), jnp.float32),
                    pltpu.VMEM((8 * OUT_ROWS, 128), jnp.float32),
                    pltpu.VMEM((ROWS, 2) + tile, jnp.float32),
                    pltpu.VMEM((2, ROWS, 2) + tile, jnp.float32),
                    pltpu.VMEM((6, 2) + tile, jnp.float32),
                    pltpu.VMEM((2, 19, ROWS) + tile, jnp.float32),
                    pltpu.VMEM((3, ROWS + 2) + tile, jnp.float32),
                    pltpu.VMEM((3, ROWS + 2) + tile, jnp.float32),
                    pltpu.VMEM((STEPS, TOTAL) + tile, jnp.float32),
                    pltpu.VMEM((STEPS, TOTAL) + tile, jnp.float32),
                    pltpu.SemaphoreType.DMA((4,)),
                    pltpu.SemaphoreType.DMA((3,)),
                    pltpu.SemaphoreType.DMA((2, 2, 7)),
                    pltpu.SemaphoreType.DMA((2, 7)),
                    pltpu.SemaphoreType.DMA((2, 8)),
                    pltpu.SemaphoreType.DMA((2, STEPS, 14)),
                ],
                compiler_params=pltpu.CompilerParams(collective_id=0, has_side_effects=True, vmem_limit_bytes=16 << 20),
            )(*(pltpu.with_memory_space_constraint(a, pltpu.HBM) for a in (density_scatter, initial_velocity, bubble_mask, wall_flags)))
        return tuple(
            pl.pallas_call(
                unpack,
                out_shape=[
                    jax.ShapeDtypeStruct(block, jnp.float32),
                    jax.ShapeDtypeStruct((3,) + block, jnp.float32),
                ],
                in_specs=[pl.BlockSpec(memory_space=pltpu.VMEM)],
                out_specs=[pl.BlockSpec(memory_space=pltpu.VMEM)] * 2,
                compiler_params=pltpu.CompilerParams(vmem_limit_bytes=4 << 20),
            )(fields)
        )

    return jax.shard_map(
        on_device,
        mesh=mesh,
        in_specs=(
            P("gx", "gy", "gz"),
            P(None, "gx", "gy", "gz"),
            P("gx", "gy", "gz"),
            P("gx", "gy", "gz"),
        ),
        out_specs=(P("gx", "gy", "gz"), P(None, "gx", "gy", "gz")),
        check_vma=False,
    )
```
